128 devices in a mesh: group: 4 (over x), shard: 32 (over z, y, core).
Axes of the slice: x: 4, y: 4, z: 4, core: 2. Of those that a mesh axis runs over, the one named last changes fastest.
Arguments:
- grad_pooled: bfloat16 [16384, 512, 128], P(('group', 'shard')), may hold values from -6 to 6
- bag_rows: int32 [16384, 512, 8], P(('group', 'shard')), may hold values from 0 to 511
- bag_lengths: int32 [16384, 512], P(('group', 'shard')), may hold values from 1 to 8
- table_order: int32 [512], replicated, may hold values from 0 to 511, each once
- weights: bfloat16 [512, 512, 128], P('shard'), may hold values from -6 to 6
- accum: float32 [512, 512], P('shard'), may hold values from 0.1 to 10
Outputs:
- new_weights: bfloat16 [512, 512, 128], P('shard')
- new_accum: float32 [512, 512], P('shard')
The draws below stay inside these ranges and needn't reach their ends.
All inputs are finite; a program needn't handle non-finite values.
Results may differ from the reference program's by a relative error of at most 0.001.
Values may be sent and summed in bfloat16 or wider, within the bound.
No kernel may reach another device: no remote copies, remote signals or barrier semaphores. Data moves between devices by JAX's collectives and lax.ppermute only.
A program may use at most 128 MiB of HBM per device.

```python
import math
import jax
import jax.numpy as jnp
from jax import lax

D = 128
TABLES = 512
ROWS = 512
BAG = 8
BATCH = 16384


def plant(values, own_key, smallest, high):
    longest = values.shape.index(max(values.shape))
    spots = []
    for shift in (0, 1):
        where = [jax.random.randint(jax.random.fold_in(own_key, axis), (), 0, length) for axis, length in enumerate(values.shape)]
        where[longest] = (where[longest] + shift) % values.shape[longest]
        spots.append(tuple(where))
    return values.at[spots[0]].set(smallest).at[spots[1]].set(high)


def steps_of(rng, dims, cuts, least, top_value):
    gain, own = 1.0, jax.random.fold_in(rng, 6)
    for axis_at, blocks in cuts:
        heights = jnp.exp(jax.random.uniform(jax.random.fold_in(own, axis_at), (blocks,), jnp.float32, least / len(cuts), top_value / len(cuts)))
        gain = gain * jnp.repeat(heights, dims[axis_at] // blocks).reshape([-1 if axis == axis_at else 1 for axis in range(len(dims))])
    return gain


def noise(own_key, shape, scale, reach, split=(), kind=jnp.bfloat16):
    level = steps_of(own_key, shape, split, -0.22, 0.18) if split else 1.0
    entries = jax.random.normal(own_key, shape, jnp.float32) * scale * level
    return jnp.minimum(jnp.maximum(entries, -reach), reach).astype(kind)


def setup_inputs(seed: int = 0) -> dict:
    seeds = jax.random.split(jax.random.key(seed), 7)
    grad_pooled = noise(seeds[0], (BATCH, TABLES, D), 1.0, 6.0, ((0, 128),))
    bag_rows = plant(jax.random.randint(seeds[1], (BATCH, TABLES, BAG), 0, ROWS), jax.random.fold_in(seeds[1], 1), 0, ROWS - 1).astype(jnp.int32)
    bag_lengths = plant(jax.random.randint(seeds[2], (BATCH, TABLES), 1, BAG + 1), jax.random.fold_in(seeds[2], 1), 1, BAG).astype(jnp.int32)
    table_order = jax.random.permutation(seeds[3], TABLES).astype(jnp.int32)
    weights = noise(seeds[4], (TABLES, ROWS, D), 1.0, 6.0, ((0, 32),))
    accum = jnp.clip(jnp.exp(math.log(10.0) - 4.6051702 * jax.random.uniform(seeds[5], (TABLES, ROWS), jnp.float32) ** steps_of(seeds[5], (TABLES, ROWS), ((0, 32),), -0.2, 0.2)), 0.1, 10.0)
    return dict(grad_pooled=grad_pooled, bag_rows=bag_rows, bag_lengths=bag_lengths, table_order=table_order, weights=weights, accum=accum)


LEARN_RATE = 0.5
EPSILON = 1e-06

def reference(grad_pooled, bag_rows, bag_lengths, table_order, weights, accum):
    pooled = jnp.take(grad_pooled, table_order, axis=1).astype(jnp.float32)
    places = jnp.arange(BAG, dtype=jnp.int32)
    live = places[None, None, :] < bag_lengths[:, :, None]
    row_ids = jnp.where(live, bag_rows, ROWS).astype(jnp.int32)
    row_ids = jnp.take(row_ids, table_order, axis=1)

    def one_table(member):
        values, chosen = member
        spread = jnp.broadcast_to(values[:, None, :], (values.shape[0], BAG, D)).reshape(-1, D)
        summed = jax.ops.segment_sum(spread, chosen.reshape(-1), num_segments=ROWS + 1)
        return summed[:ROWS]
    row_grad = lax.map(one_table, (jnp.swapaxes(pooled, 0, 1), jnp.swapaxes(row_ids, 0, 1)))
    new_accum = accum + lax.optimization_barrier(jnp.mean(row_grad * row_grad, axis=-1))
    step_size = LEARN_RATE / (jnp.sqrt(new_accum) + EPSILON)
    new_weights = (weights.astype(jnp.float32) - step_size[:, :, None] * row_grad).astype(jnp.bfloat16)
    return (new_weights, new_accum)
```

```python
import functools

import jax
import jax.numpy as jnp
from jax import lax
from jax.experimental import pallas as pl
from jax.experimental.pallas import tpu as pltpu
from jax.sharding import PartitionSpec as P

LEARN_RATE = 0.5
EPSILON = 1e-06
LANES = 128
TILE = 16
DIGIT = 64


def pack_kernel(where_ref, turn_ref, grad_ref, rows_ref, lens_ref, out_ref,
                codes, stage, id_stage, stage_sem, id_sem):
    samples, bag, tables = rows_ref.shape
    step = pl.program_id(0)
    steps = pl.num_programs(0)
    slot = lax.rem(step, 2)

    def table_copy(which, t, step_now):
        place = where_ref[step_now * TILE + t]
        dest = lax.div(place, 4)
        q = lax.rem(place, 4)
        return pltpu.make_async_copy(
            stage.at[which, t],
            out_ref.at[dest, pl.ds(pl.multiple_of(q * samples, samples), samples), :],
            stage_sem.at[which, t],
        )

    def id_copy(t):
        place = where_ref[t]
        dest = lax.div(place, 4)
        q = lax.rem(place, 4)
        return pltpu.make_async_copy(
            id_stage.at[t],
            out_ref.at[dest, pl.ds(pl.multiple_of(4 * samples + q * bag, bag), bag), :],
            id_sem,
        )

    @pl.when(step >= 2)
    def _():
        for t in range(TILE):
            table_copy(slot, t, step - 2).wait()

    turn = turn_ref[...]
    for pair in range(samples // (2 * TILE)):
        first = grad_ref[pl.ds(2 * pair * TILE, TILE)].reshape(TILE * TILE, LANES)
        second = grad_ref[pl.ds((2 * pair + 1) * TILE, TILE)].reshape(TILE * TILE, LANES)
        both = jnp.concatenate([first, second], axis=1)
        turned = jnp.dot(turn, both, preferred_element_type=jnp.float32).astype(jnp.bfloat16)
        for half in range(2):
            part = turned[:, half * LANES:(half + 1) * LANES].reshape(TILE, TILE, LANES)
            stage[slot, :, pl.ds((2 * pair + half) * TILE, TILE), :] = part

    for t in range(TILE):
        table_copy(slot, t, step).start()

    @pl.when(step == 0)
    def _():
        for block in range(tables // LANES):
            span = pl.ds(block * LANES, LANES)
            lens = lens_ref[:, span]
            for j in range(bag):
                ids = rows_ref[:, j, span]
                code = jnp.left_shift(DIGIT + (ids & (DIGIT - 1)), ids >> 6)
                code = jnp.where(lens > j, code, 0).astype(jnp.float32)
                codes[pl.ds(block * LANES * bag + j, LANES, stride=bag), :] = code.T
        id_stage[...] = codes[...].reshape(tables, bag, LANES).astype(jnp.bfloat16)

        def send(t, carry):
            id_copy(t).start()
            return carry
        lax.fori_loop(0, tables, send, 0)

    @pl.when(step == steps - 1)
    def _():
        for t in range(TILE):
            table_copy(1 - slot, t, step - 1).wait()
        for t in range(TILE):
            table_copy(slot, t, step).wait()

        def settle(t, carry):
            id_copy(t).wait()
            return carry
        lax.fori_loop(0, tables, settle, 0)


def pack_tables(grad, rows, lens, places):
    samples, tables, width = grad.shape
    bag = rows.shape[1]
    devices = tables // 4
    index = jnp.arange(TILE * TILE, dtype=jnp.int32)
    source = (index % TILE) * TILE + index // TILE
    turn = (source[:, None] == index[None, :]).astype(jnp.bfloat16)
    return pl.pallas_call(
        pack_kernel,
        out_shape=jax.ShapeDtypeStruct((devices, 4 * (samples + bag), width), jnp.bfloat16),
        grid_spec=pltpu.PrefetchScalarGridSpec(
            num_scalar_prefetch=1,
            grid=(tables // TILE,),
            in_specs=[
                pl.BlockSpec((TILE * TILE, TILE * TILE), lambda i, w: (0, 0)),
                pl.BlockSpec((samples, TILE, width), lambda i, w: (0, i, 0)),
                pl.BlockSpec((samples, bag, tables), lambda i, w: (0, 0, 0)),
                pl.BlockSpec((samples, tables), lambda i, w: (0, 0)),
            ],
            out_specs=pl.BlockSpec(memory_space=pl.ANY),
            scratch_shapes=[
                pltpu.VMEM((tables * bag, LANES), jnp.float32),
                pltpu.VMEM((2, TILE, samples, width), jnp.bfloat16),
                pltpu.VMEM((tables, bag, LANES), jnp.bfloat16),
                pltpu.SemaphoreType.DMA((2, TILE)),
                pltpu.SemaphoreType.DMA,
            ],
        ),
        compiler_params=pltpu.CompilerParams(dimension_semantics=("arbitrary",)),
        name="pack_tables",
    )(places, turn, grad, rows, lens)


def decode(code):
    level = jnp.ones(code.shape, jnp.int32)
    big = code >= 1024.0
    code = jnp.where(big, code * 0.0625, code)
    level = jnp.where(big, jnp.left_shift(level, 16), level)
    big = code >= 256.0
    code = jnp.where(big, code * 0.25, code)
    level = jnp.where(big, jnp.left_shift(level, 8), level)
    big = code >= 128.0
    code = jnp.where(big, code * 0.5, code)
    level = jnp.where(big, jnp.left_shift(level, 4), level)
    return code.astype(jnp.int32) - DIGIT, level


def count_rows(low_ref, level_ref, counts, group, column, bag):
    sublane = lax.broadcasted_iota(jnp.int32, (DIGIT, LANES), 0)
    word = jnp.zeros((DIGIT, LANES), jnp.int32)
    for j in range(bag):
        row = group * bag + j
        low = low_ref[pl.ds(row, DIGIT, stride=0), :]
        level = level_ref[pl.ds(row, DIGIT, stride=0), :]
        word = word + jnp.where(low == sublane, level, 0)
    for digit in range(8):
        count = (lax.shift_right_logical(word, 4 * digit) & 15).astype(jnp.float32)
        counts[digit * DIGIT:(digit + 1) * DIGIT, column * LANES:(column + 1) * LANES] = (
            count.astype(jnp.bfloat16)
        )


def update_kernel(start_ref, grad_ref, code_ref, weight_ref, accum_ref, out_w, out_a,
                  total, low_ref, level_ref, counts_a, counts_b):
    block = pl.program_id(1)
    sources, bag = code_ref.shape[0], code_ref.shape[1]
    row_count = total.shape[0]

    @pl.when(block == 0)
    def _():
        total[...] = jnp.zeros_like(total)

    low, level = decode(code_ref[...].astype(jnp.float32))
    low_ref[...] = low.reshape(sources * bag, LANES)
    level_ref[...] = level.reshape(sources * bag, LANES)

    per = counts_a.shape[1] // LANES
    held = (counts_a, counts_b)
    chunks = sources // per
    for chunk in range(chunks + 1):
        if chunk < chunks:
            for column in range(per):
                count_rows(low_ref, level_ref, held[chunk % 2], chunk * per + column, column, bag)
        if chunk > 0:
            values = grad_ref[(chunk - 1) * per:chunk * per].reshape(per * LANES, LANES)
            total[...] += jnp.dot(
                held[(chunk - 1) % 2][...], values, preferred_element_type=jnp.float32
            )

    @pl.when(block == pl.num_programs(1) - 1)
    def _():
        row_grad = total[...]
        mean = jnp.sum(row_grad * row_grad, axis=1, keepdims=True) * (1.0 / LANES)
        old = jnp.broadcast_to(accum_ref[0], (LANES, row_count)).T
        new = old + mean
        step_size = LEARN_RATE / (jnp.sqrt(new) + EPSILON)
        out_w[0] = (weight_ref[0].astype(jnp.float32) - step_size * row_grad).astype(out_w.dtype)
        out_a[0] = new.T[0:1, :]


def update_tables(received, weights, accum, start, quarter, samples, bag):
    devices = received.shape[0]
    row_count, width = weights.shape[1], weights.shape[2]
    sources = 16
    per = 4
    first_code = (4 * samples) // bag
    return pl.pallas_call(
        update_kernel,
        out_shape=(
            jax.ShapeDtypeStruct((quarter, row_count, width), jnp.bfloat16),
            jax.ShapeDtypeStruct((quarter, 1, row_count), jnp.float32),
        ),
        grid_spec=pltpu.PrefetchScalarGridSpec(
            num_scalar_prefetch=1,
            grid=(quarter, devices // sources),
            in_specs=[
                pl.BlockSpec((sources, samples, width), lambda q, k, s: (k, q, 0)),
                pl.BlockSpec((sources, bag, width), lambda q, k, s: (k, first_code + q, 0)),
                pl.BlockSpec((1, row_count, width), lambda q, k, s: (s[0] + q, 0, 0)),
                pl.BlockSpec((1, 1, row_count), lambda q, k, s: (s[0] + q, 0, 0)),
            ],
            out_specs=(
                pl.BlockSpec((1, row_count, width), lambda q, k, s: (q, 0, 0)),
                pl.BlockSpec((1, 1, row_count), lambda q, k, s: (q, 0, 0)),
            ),
            scratch_shapes=[
                pltpu.VMEM((row_count, width), jnp.float32),
                pltpu.VMEM((sources * bag, LANES), jnp.int32),
                pltpu.VMEM((sources * bag, LANES), jnp.int32),
                pltpu.VMEM((row_count, per * LANES), jnp.bfloat16),
                pltpu.VMEM((row_count, per * LANES), jnp.bfloat16),
            ],
        ),
        compiler_params=pltpu.CompilerParams(dimension_semantics=("arbitrary", "arbitrary")),
        name="update_tables",
    )(start, received, received, weights, accum[:, None, :])


def table_places(table_order, groups, shards, quarter):
    tables = table_order.shape[0]
    source = table_order.reshape(shards, groups, quarter).transpose(1, 0, 2).reshape(tables)
    index = jnp.arange(tables, dtype=jnp.int32)
    return jnp.sum(jnp.where(source[None, :] == index[:, None], index[None, :], 0), axis=1)


def body(grad_pooled, bag_rows, bag_lengths, table_order, weights, accum):
    bag = bag_rows.shape[2]
    samples = grad_pooled.shape[0]
    groups = lax.axis_size("group")
    shards = lax.axis_size("shard")
    quarter = weights.shape[0] // groups
    places = table_places(table_order, groups, shards, quarter)
    packed = pack_tables(grad_pooled, jnp.transpose(bag_rows, (0, 2, 1)), bag_lengths, places)
    received = lax.all_to_all(packed, ("group", "shard"), split_axis=0, concat_axis=0, tiled=True)
    start = (lax.axis_index("group") * quarter).astype(jnp.int32).reshape(1)
    part_weights, part_accum = update_tables(
        received, weights, accum, start, quarter, samples, bag
    )
    full_weights = lax.all_gather(part_weights, "group", axis=0, tiled=True)
    full_accum = lax.all_gather(part_accum[:, 0, :], "group", axis=0, tiled=True)
    return (full_weights, full_accum)


def solution(mesh):
    in_specs = (
        P(("group", "shard"), None, None),
        P(("group", "shard"), None, None),
        P(("group", "shard"), None),
        P(),
        P("shard", None, None),
        P("shard", None),
    )
    out_specs = (P("shard", None, None), P("shard", None))
    return jax.shard_map(body, mesh=mesh, in_specs=in_specs, out_specs=out_specs, check_vma=False)
```

```python
import functools

import jax
import jax.numpy as jnp
from jax import lax
from jax.experimental import pallas as pl
from jax.experimental.pallas import tpu as pltpu
from jax.sharding import PartitionSpec as P

LEARN_RATE = 0.5
EPSILON = 1e-06
LANES = 128
TILE = 16
DIGIT = 64
SIDE = 4
AXES = ("group", "shard")
ROUTES = ("xyz", "yzx", "zyx", "xzy")
UNIT = 1048576.0
LIMIT = 32767.0


def device_of(x, z, y, c):
    return x * 32 + (z * SIDE + y) * 2 + c


def shift(value, axis, by, flip=0):
    pairs = []
    for x in range(SIDE):
        for z in range(SIDE):
            for y in range(SIDE):
                for c in range(2):
                    to = {"x": x, "y": y, "z": z}
                    to[axis] = (to[axis] + by) % SIDE
                    pairs.append((device_of(x, z, y, c), device_of(to["x"], to["z"], to["y"], c ^ flip)))
    return lax.ppermute(value, AXES, pairs)


def pack_kernel(order_ref, here_ref, turn_ref, grad_ref, rows_ref, lens_ref, *rest):
    outs, (codes, stage, id_stage, sem) = rest[:32], rest[32:]
    samples, bag, tables = rows_ref.shape
    step = pl.program_id(0)

    turn = turn_ref[...]
    for pair in range(samples // (2 * TILE)):
        first = grad_ref[pl.ds(2 * pair * TILE, TILE)].reshape(TILE * TILE, LANES)
        second = grad_ref[pl.ds((2 * pair + 1) * TILE, TILE)].reshape(TILE * TILE, LANES)
        both = jnp.concatenate([first, second], axis=1)
        turned = jnp.dot(turn, both, preferred_element_type=jnp.float32).astype(jnp.bfloat16)
        for half in range(2):
            part = turned[:, half * LANES:(half + 1) * LANES].reshape(TILE, TILE, LANES)
            stage[pl.ds(step * TILE, TILE), pl.ds((2 * pair + half) * TILE, TILE), :] = part

    @pl.when(step == 0)
    def _():
        for block in range(tables // LANES):
            span = pl.ds(block * LANES, LANES)
            lens = lens_ref[:, span]
            for j in range(bag):
                ids = rows_ref[:, j, span]
                code = jnp.left_shift(DIGIT + (ids & (DIGIT - 1)), ids >> 6)
                code = jnp.where(lens > j, code, 0).astype(jnp.float32)
                codes[pl.ds(block * LANES * bag + j, LANES, stride=bag), :] = code.T

    def table_at(message, i):
        route = ROUTES[message // 8]
        place = {"x": here_ref[0], "z": here_ref[1], "y": here_ref[2]}
        moves = ((message % 8) // 2, lax.shift_right_logical(i, 2), i & 3)
        for axis, by in zip(route, moves):
            place[axis] = (place[axis] + by) & 3
        core = here_ref[3] ^ (message % 2)
        shard = (place["z"] * SIDE + place["y"]) * 2 + core
        return order_ref[shard * 16 + place["x"] * SIDE + message // 8]

    def table_copy(message, i, table):
        return pltpu.make_async_copy(
            stage.at[table],
            outs[message].at[pl.ds(pl.multiple_of(i * samples, samples), samples), :],
            sem.at[message],
        )

    def id_copy(message):
        return pltpu.make_async_copy(
            id_stage.at[message],
            outs[message].at[pl.ds(TILE * samples, TILE * bag), :],
            sem.at[message],
        )

    @pl.when(step == pl.num_programs(0) - 1)
    def _():
        for message in range(32):
            def send(half, carry):
                pieces = []
                for odd in range(2):
                    i = half * 2 + odd
                    table = table_at(message, i)
                    table_copy(message, i, table).start()
                    pieces.append(codes[pl.ds(pl.multiple_of(table * bag, bag), bag), :])
                both = jnp.concatenate(pieces, axis=0).astype(jnp.bfloat16)
                id_stage[message, pl.ds(pl.multiple_of(half * 2 * bag, 2 * bag), 2 * bag), :] = both
                return carry
            lax.fori_loop(0, TILE // 2, send, 0)
            id_copy(message).start()
        for message in range(32):
            def settle(i, carry):
                table_copy(message, i, 0).wait()
                return carry
            lax.fori_loop(0, TILE, settle, 0)
            id_copy(message).wait()


def pack_tables(grad, rows, lens, order, here):
    samples, tables, width = grad.shape
    bag = rows.shape[1]
    index = jnp.arange(TILE * TILE, dtype=jnp.int32)
    source = (index % TILE) * TILE + index // TILE
    turn = (source[:, None] == index[None, :]).astype(jnp.bfloat16)
    message = jax.ShapeDtypeStruct((TILE * (samples + bag), width), jnp.bfloat16)
    return pl.pallas_call(
        pack_kernel,
        out_shape=(message,) * 32,
        grid_spec=pltpu.PrefetchScalarGridSpec(
            num_scalar_prefetch=2,
            grid=(tables // TILE,),
            in_specs=[
                pl.BlockSpec((TILE * TILE, TILE * TILE), lambda i, o, h: (0, 0)),
                pl.BlockSpec((samples, TILE, width), lambda i, o, h: (0, i, 0)),
                pl.BlockSpec((samples, bag, tables), lambda i, o, h: (0, 0, 0)),
                pl.BlockSpec((samples, tables), lambda i, o, h: (0, 0)),
            ],
            out_specs=(pl.BlockSpec(memory_space=pl.ANY),) * 32,
            scratch_shapes=[
                pltpu.VMEM((tables * bag, LANES), jnp.float32),
                pltpu.VMEM((tables, samples, width), jnp.bfloat16),
                pltpu.VMEM((32, TILE * bag, LANES), jnp.bfloat16),
                pltpu.SemaphoreType.DMA((32,)),
            ],
        ),
        compiler_params=pltpu.CompilerParams(dimension_semantics=("arbitrary",)),
        name="pack_tables",
    )(order, here, turn, grad, rows, lens)


def decode(code):
    level = jnp.ones(code.shape, jnp.int32)
    big = code >= 1024.0
    code = jnp.where(big, code * 0.0625, code)
    level = jnp.where(big, jnp.left_shift(level, 16), level)
    big = code >= 256.0
    code = jnp.where(big, code * 0.25, code)
    level = jnp.where(big, jnp.left_shift(level, 8), level)
    big = code >= 128.0
    code = jnp.where(big, code * 0.5, code)
    level = jnp.where(big, jnp.left_shift(level, 4), level)
    return code.astype(jnp.int32) - DIGIT, level


def count_rows(low_ref, level_ref, counts, first, column, bag):
    sublane = lax.broadcasted_iota(jnp.int32, (DIGIT, LANES), 0)
    word = jnp.zeros((DIGIT, LANES), jnp.int32)
    for j in range(bag):
        low = low_ref[pl.ds(first + j, DIGIT, stride=0), :]
        level = level_ref[pl.ds(first + j, DIGIT, stride=0), :]
        word = word + jnp.where(low == sublane, level, 0)
    for digit in range(8):
        count = (lax.shift_right_logical(word, 4 * digit) & 15).astype(jnp.float32)
        counts[digit * DIGIT:(digit + 1) * DIGIT, column * LANES:(column + 1) * LANES] = (
            count.astype(jnp.bfloat16)
        )


def diagonal():
    shape = (LANES, LANES)
    return lax.broadcasted_iota(jnp.int32, shape, 0) == lax.broadcasted_iota(jnp.int32, shape, 1)


def as_row(column):
    return jnp.sum(jnp.where(diagonal(), column, 0.0), axis=0, keepdims=True)


def as_column(row):
    return jnp.sum(jnp.where(diagonal(), row, 0.0), axis=1, keepdims=True)


def narrow(block):
    most = jnp.max(jnp.abs(block), axis=1, keepdims=True)
    units = jnp.floor(most * (UNIT / LIMIT)) + 1.0
    return jnp.round(block * (UNIT / units)).astype(jnp.int32), as_row(units).astype(jnp.int32)


def narrow_table(read, put_words, put_units):
    for pair in range(2):
        low, low_units = narrow(read(pair))
        high, high_units = narrow(read(pair + 2))
        put_words(pair, (low & 65535) | jnp.left_shift(high, 16))
        put_units(pair, low_units)
        put_units(pair + 2, high_units)


def widen(ref, tables, table, block):
    words = ref[(table * 2 + block % 2) * LANES:(table * 2 + block % 2 + 1) * LANES, :]
    if block < 2:
        words = jnp.left_shift(words, 16)
    numbers = jnp.right_shift(words, 16).astype(jnp.float32)
    at = tables * 2 * LANES + table * 4 + block
    units = as_column(ref[at:at + 1, :].astype(jnp.float32))
    return numbers * (units * (1.0 / UNIT))


def gather_kernel(*refs):
    values, codes = refs[:8], refs[8:16]
    outs, (low_ref, level_ref, counts_a, counts_b, held) = refs[16:20], refs[20:]
    step = pl.program_id(0)
    bag = 8
    for k in range(8):
        low, level = decode(codes[k][...].astype(jnp.float32))
        low_ref[k * 2 * bag:(k + 1) * 2 * bag, :] = low
        level_ref[k * 2 * bag:(k + 1) * 2 * bag, :] = level
    for t in range(2):
        total = None
        for half, counts in enumerate((counts_a, counts_b)):
            for column in range(4):
                k = half * 4 + column
                count_rows(low_ref, level_ref, counts, k * 2 * bag + t * bag, column, bag)
            rows = jnp.concatenate(
                [values[half * 4 + n][t * LANES:(t + 1) * LANES, :] for n in range(4)], axis=0
            )
            term = jnp.dot(counts[...], rows, preferred_element_type=jnp.float32)
            if half == 0:
                held[t] = term
            else:
                held[t] = held[t] + term
    for t in range(2):
        table = lax.rem(step, 2) * 2 + t
        for target in range(SIDE):
            @pl.when(lax.div(step, 2) == target)
            def _():
                def put_words(pair, words):
                    at = pl.multiple_of(table * 256 + pair * LANES, LANES)
                    outs[target][pl.ds(at, LANES), :] = words

                def put_units(block, units):
                    outs[target][pl.ds(SIDE * 256 + table * 4 + block, 1), :] = units

                narrow_table(
                    lambda block: held[t, block * LANES:(block + 1) * LANES, :],
                    put_words, put_units,
                )


def sum_line(messages):
    rows = messages[0].shape[0]
    samples, bag = LANES, 8
    width = messages[0].shape[1]
    out = jax.ShapeDtypeStruct((SIDE * 260, width), jnp.int32)
    return pl.pallas_call(
        gather_kernel,
        out_shape=(out,) * SIDE,
        grid=(8,),
        in_specs=(
            [pl.BlockSpec((2 * samples, width), lambda i: (i, 0))] * 8
            + [pl.BlockSpec((2 * bag, width), lambda i: (TILE * samples // (2 * bag) + i, 0))] * 8
        ),
        out_specs=(pl.BlockSpec((SIDE * 260, width), lambda i: (0, 0)),) * SIDE,
        scratch_shapes=[
            pltpu.VMEM((128, LANES), jnp.int32),
            pltpu.VMEM((128, LANES), jnp.int32),
            pltpu.VMEM((512, 512), jnp.bfloat16),
            pltpu.VMEM((512, 512), jnp.bfloat16),
            pltpu.VMEM((2, 512, LANES), jnp.float32),
        ],
        compiler_params=pltpu.CompilerParams(dimension_semantics=("arbitrary",)),
        cost_estimate=pl.CostEstimate(
            flops=16 * 2 * 512 * 1024 * 128, bytes_accessed=8 * rows * 256, transcendentals=0
        ),
        name="sum_line",
    )(*messages, *messages)


def merge_kernel(*refs):
    ins, outs = refs[:SIDE], refs[SIDE:]
    for table in range(SIDE):
        out = outs[table]

        def read(block):
            return sum(widen(ref, SIDE, table, block) for ref in ins)

        def put_words(pair, words):
            out[pair * LANES:(pair + 1) * LANES, :] = words

        def put_units(block, units):
            out[256 + block:257 + block, :] = units

        narrow_table(read, put_words, put_units)
        out[260:264, :] = jnp.zeros((4, LANES), jnp.int32)


def merge_tables(parts):
    out = jax.ShapeDtypeStruct((264, LANES), jnp.int32)
    return pl.pallas_call(
        merge_kernel,
        out_shape=(out,) * SIDE,
        cost_estimate=pl.CostEstimate(
            flops=20_000_000, bytes_accessed=5 * 532480, transcendentals=0
        ),
        name="merge_tables",
    )(*parts)


def finish_kernel(count, start_ref, *refs):
    sums, weights = refs[:SIDE * count], refs[SIDE * count:(SIDE + 1) * count]
    accums = refs[(SIDE + 1) * count:(SIDE + 2) * count]
    out, rows = refs[(SIDE + 2) * count:]
    for n in range(count):
        for block in range(4):
            grad = sum(widen(ref, 1, 0, block) for ref in sums[n * SIDE:(n + 1) * SIDE])
            span = slice(block * LANES, (block + 1) * LANES)
            mean = jnp.sum(grad * grad, axis=1, keepdims=True) * (1.0 / LANES)
            new = as_column(accums[n][0, :, span]) + mean
            step_size = LEARN_RATE / (jnp.sqrt(new) + EPSILON)
            old = weights[n][0, span, :].astype(jnp.float32)
            at = n * 528 + block * LANES
            out[at:at + LANES, :] = (old - step_size * grad).astype(out.dtype)
            left = as_row(new)
            for piece in range(3):
                head = left.astype(jnp.bfloat16).astype(jnp.float32)
                rows[piece * 4 + block:piece * 4 + block + 1, :] = head
                left = left - head
        rows[12:16, :] = jnp.zeros((4, LANES), jnp.float32)
        out[n * 528 + 512:n * 528 + 528, :] = rows[...].astype(out.dtype)


def finish(sums, weights, accum, start, quarters):
    count = len(quarters)
    rows = weights.shape[1]
    flat = [piece for group in sums for piece in group]

    def at(q):
        return lambda i, s: (s[0] + q, 0, 0)

    return pl.pallas_call(
        functools.partial(finish_kernel, count),
        out_shape=jax.ShapeDtypeStruct((count * 528, LANES), jnp.bfloat16),
        grid_spec=pltpu.PrefetchScalarGridSpec(
            num_scalar_prefetch=1,
            grid=(1,),
            in_specs=(
                [pl.BlockSpec((264, LANES), lambda i, s: (0, 0))] * (SIDE * count)
                + [pl.BlockSpec((1, rows, LANES), at(q)) for q in quarters]
                + [pl.BlockSpec((1, 1, rows), at(q)) for q in quarters]
            ),
            out_specs=pl.BlockSpec((count * 528, LANES), lambda i, s: (0, 0)),
            scratch_shapes=[pltpu.VMEM((16, LANES), jnp.float32)],
        ),
        compiler_params=pltpu.CompilerParams(dimension_semantics=("arbitrary",)),
        cost_estimate=pl.CostEstimate(
            flops=10_000_000, bytes_accessed=count * 900_000, transcendentals=0
        ),
        name="finish",
    )(start, *flat, *([weights] * count), *([accum] * count))


def place_kernel(layout, x_ref, *refs):
    ins, (out_w, out_a) = refs[:-2], refs[-2:]
    for group, quarters in enumerate(layout):
        for by in range(SIDE):
            ref = ins[group * SIDE + by]
            base = ((x_ref[0] + SIDE - by) & 3) * SIDE
            for n, q in enumerate(quarters):
                out_w[base + q] = ref[n * 528:n * 528 + 512, :]
                pieces = ref[n * 528 + 512:n * 528 + 528, :].astype(jnp.float32)
                out_a[base + q] = (pieces[0:4, :] + pieces[4:8, :]) + pieces[8:12, :]


def place(messages, layout, x, slots, rows):
    return pl.pallas_call(
        functools.partial(place_kernel, layout),
        out_shape=(
            jax.ShapeDtypeStruct((slots, rows, LANES), jnp.bfloat16),
            jax.ShapeDtypeStruct((slots, 4, LANES), jnp.float32),
        ),
        in_specs=[pl.BlockSpec(memory_space=pltpu.SMEM)]
        + [pl.BlockSpec(memory_space=pltpu.VMEM)] * len(messages),
        out_specs=(pl.BlockSpec(memory_space=pltpu.VMEM),) * 2,
        name="place",
    )(x, *messages)


def body(grad_pooled, bag_rows, bag_lengths, table_order, weights, accum):
    x = lax.axis_index("group").astype(jnp.int32)
    shard = lax.axis_index("shard").astype(jnp.int32)
    here = jnp.stack([x, shard // 8, (shard // 2) % 4, shard % 2]).astype(jnp.int32)
    messages = pack_tables(
        grad_pooled, jnp.transpose(bag_rows, (0, 2, 1)), bag_lengths, table_order, here
    )
    arrived = []
    for part, route in enumerate(ROUTES):
        line = []
        for k in range(8):
            sent = messages[part * 8 + k]
            line.append(sent if k == 0 else shift(sent, route[0], k // 2, k % 2))
        arrived.append(line)
    sums = []
    for part, route in enumerate(ROUTES):
        partial = sum_line(arrived[part])
        partial = [partial[0]] + [shift(partial[by], route[1], by) for by in range(1, SIDE)]
        merged = merge_tables(partial)
        merged = [merged[0]] + [shift(merged[by], route[2], by) for by in range(1, SIDE)]
        sums.append(merged)
    layout = ((0, 1, 2), (3,))
    start = (x * SIDE).reshape(1)
    accum_rows = accum[:, None, :]
    final = []
    for quarters in layout:
        mine = finish([sums[q] for q in quarters], weights, accum_rows, start, quarters)
        final += [mine] + [shift(mine, "x", by) for by in range(1, SIDE)]
    new_weights, new_accum = place(
        final, layout, x.reshape(1), weights.shape[0], weights.shape[1]
    )
    return (new_weights, new_accum.reshape(accum.shape))


def solution(mesh):
    in_specs = (
        P(("group", "shard"), None, None),
        P(("group", "shard"), None, None),
        P(("group", "shard"), None),
        P(),
        P("shard", None, None),
        P("shard", None),
    )
    out_specs = (P("shard", None, None), P("shard", None))
    return jax.shard_map(body, mesh=mesh, in_specs=in_specs, out_specs=out_specs, check_vma=False)
```

```python
import functools

import jax
import jax.numpy as jnp
from jax import lax
from jax.experimental import pallas as pl
from jax.experimental.pallas import tpu as pltpu
from jax.sharding import PartitionSpec as P

LEARN_RATE = 0.5
EPSILON = 1e-06
LANES = 128
TILE = 16
DIGIT = 64
SIDE = 4
AXES = ("group", "shard")
ROUTES = ("xyz", "yzx", "zyx", "xzy")
REACH = 32500.0
UNIT = 1024.0


def device_of(x, z, y, c):
    return x * 32 + (z * SIDE + y) * 2 + c


def shift(value, axis, by, flip=0):
    pairs = []
    for x in range(SIDE):
        for z in range(SIDE):
            for y in range(SIDE):
                for c in range(2):
                    to = {"x": x, "y": y, "z": z}
                    to[axis] = (to[axis] + by) % SIDE
                    pairs.append((device_of(x, z, y, c), device_of(to["x"], to["z"], to["y"], c ^ flip)))
    return lax.ppermute(value, AXES, pairs)


def pack_kernel(order_ref, here_ref, grad_ref, rows_ref, lens_ref, *rest):
    outs, (codes, stage, id_stage, turn_ref, sem) = rest[:32], rest[32:]
    samples, bag, tables = rows_ref.shape
    step = pl.program_id(0)

    @pl.when(step == 0)
    def _():
        shape = (TILE * TILE, TILE * TILE)
        row = lax.broadcasted_iota(jnp.int32, shape, 0)
        source = (row & (TILE - 1)) * TILE + lax.shift_right_logical(row, 4)
        same = source == lax.broadcasted_iota(jnp.int32, shape, 1)
        turn_ref[...] = jnp.where(same, 1.0, 0.0).astype(jnp.bfloat16)

    turn = turn_ref[...]

    def turn_pair(pair, carry):
        at = pl.multiple_of(pair * 2 * TILE, 2 * TILE)
        first = grad_ref[:, pl.ds(at, TILE), :].reshape(TILE * TILE, LANES)
        second = grad_ref[:, pl.ds(at + TILE, TILE), :].reshape(TILE * TILE, LANES)
        both = jnp.concatenate([first, second], axis=1)
        turned = jnp.dot(turn, both, preferred_element_type=jnp.float32).astype(jnp.bfloat16)
        for half in range(2):
            part = turned[:, half * LANES:(half + 1) * LANES].reshape(TILE, TILE, LANES)
            here = pl.ds(pl.multiple_of(step * TILE, TILE), TILE)
            stage[pl.ds(at + half * TILE, TILE), here, :] = part
        return carry

    lax.fori_loop(0, tables // (2 * TILE), turn_pair, 0, unroll=4)

    @pl.when(step == 0)
    def _():
        def encode(block, carry):
            span = pl.ds(pl.multiple_of(block * LANES, LANES), LANES)
            lens = lens_ref[:, span]
            for j in range(bag):
                ids = rows_ref[:, j, span]
                code = jnp.left_shift(DIGIT + (ids & (DIGIT - 1)), ids >> 6)
                code = jnp.where(lens > j, code, 0).astype(jnp.float32)
                codes[pl.ds(block * LANES * bag + j, LANES, stride=bag), :] = code.T
            return carry

        lax.fori_loop(0, tables // LANES, encode, 0)

    def table_at(message, i):
        route = ROUTES[message // 8]
        place = {"x": here_ref[0], "z": here_ref[1], "y": here_ref[2]}
        moves = ((message % 8) // 2, lax.shift_right_logical(i, 2), i & 3)
        for axis, by in zip(route, moves):
            place[axis] = (place[axis] + by) & 3
        core = here_ref[3] ^ (message % 2)
        shard = (place["z"] * SIDE + place["y"]) * 2 + core
        return order_ref[shard * 16 + place["x"] * SIDE + message // 8]

    def table_copy(message, i, table):
        return pltpu.make_async_copy(
            stage.at[table],
            outs[message].at[pl.ds(pl.multiple_of(i * samples, samples), samples), :],
            sem.at[message],
        )

    def id_copy(message):
        return pltpu.make_async_copy(
            id_stage.at[message],
            outs[message].at[pl.ds(TILE * samples, TILE * bag), :],
            sem.at[message],
        )

    @pl.when(step == pl.num_programs(0) - 1)
    def _():
        for message in range(32):
            def send(half, carry):
                pieces = []
                for odd in range(2):
                    i = half * 2 + odd
                    table = table_at(message, i)
                    table_copy(message, i, table).start()
                    pieces.append(codes[pl.ds(pl.multiple_of(table * bag, bag), bag), :])
                both = jnp.concatenate(pieces, axis=0).astype(jnp.bfloat16)
                id_stage[message, pl.ds(pl.multiple_of(half * 2 * bag, 2 * bag), 2 * bag), :] = both
                return carry
            lax.fori_loop(0, TILE // 2, send, 0)
            id_copy(message).start()
        for message in range(32):
            def settle(i, carry):
                table_copy(message, i, 0).wait()
                return carry
            lax.fori_loop(0, TILE, settle, 0)
            id_copy(message).wait()


def pack_tables(grad, rows, lens, order, here):
    samples, tables, width = grad.shape
    bag = rows.shape[1]
    message = jax.ShapeDtypeStruct((TILE * (samples + bag), width), jnp.bfloat16)
    return pl.pallas_call(
        pack_kernel,
        out_shape=(message,) * 32,
        grid_spec=pltpu.PrefetchScalarGridSpec(
            num_scalar_prefetch=2,
            grid=(samples // TILE,),
            in_specs=[
                pl.BlockSpec((TILE, tables, width), lambda i, o, h: (i, 0, 0)),
                pl.BlockSpec((samples, bag, tables), lambda i, o, h: (0, 0, 0)),
                pl.BlockSpec((samples, tables), lambda i, o, h: (0, 0)),
            ],
            out_specs=(pl.BlockSpec(memory_space=pl.ANY),) * 32,
            scratch_shapes=[
                pltpu.VMEM((tables * bag, LANES), jnp.float32),
                pltpu.VMEM((tables, samples, width), jnp.bfloat16),
                pltpu.VMEM((32, TILE * bag, LANES), jnp.bfloat16),
                pltpu.VMEM((TILE * TILE, TILE * TILE), jnp.bfloat16),
                pltpu.SemaphoreType.DMA((32,)),
            ],
        ),
        compiler_params=pltpu.CompilerParams(dimension_semantics=("arbitrary",)),
        name="pack_tables",
    )(order, here, grad, rows, lens)


def decode(code):
    level = jnp.ones(code.shape, jnp.int32)
    big = code >= 1024.0
    code = jnp.where(big, code * 0.0625, code)
    level = jnp.where(big, jnp.left_shift(level, 16), level)
    big = code >= 256.0
    code = jnp.where(big, code * 0.25, code)
    level = jnp.where(big, jnp.left_shift(level, 8), level)
    big = code >= 128.0
    code = jnp.where(big, code * 0.5, code)
    level = jnp.where(big, jnp.left_shift(level, 4), level)
    return code.astype(jnp.int32) - DIGIT, level


def count_rows(low_ref, level_ref, counts, first, column, bag):
    sublane = lax.broadcasted_iota(jnp.int32, (DIGIT, LANES), 0)
    word = jnp.zeros((DIGIT, LANES), jnp.int32)
    for j in range(bag):
        low = low_ref[pl.ds(first + j, DIGIT, stride=0), :]
        level = level_ref[pl.ds(first + j, DIGIT, stride=0), :]
        word = word + jnp.where(low == sublane, level, 0)
    for digit in range(8):
        if digit < 7:
            count = (word & (15 << (4 * digit))).astype(jnp.float32)
        else:
            count = lax.shift_right_logical(word, 28).astype(jnp.float32)
        counts[digit * DIGIT:(digit + 1) * DIGIT, column * LANES:(column + 1) * LANES] = (
            count.astype(jnp.bfloat16)
        )


def diagonal():
    shape = (LANES, LANES)
    return lax.broadcasted_iota(jnp.int32, shape, 0) == lax.broadcasted_iota(jnp.int32, shape, 1)


def as_row(column):
    return jnp.sum(jnp.where(diagonal(), column, 0.0), axis=0, keepdims=True)


def as_column(row):
    return jnp.sum(jnp.where(diagonal(), row, 0.0), axis=1, keepdims=True)


def narrow_table(read, put_words, put_peak):
    peak = None
    for block in range(8):
        values = jnp.abs(read(block)).reshape(8, 8, LANES)
        most = jnp.max(values, axis=0)
        peak = most if peak is None else jnp.maximum(peak, most)
    units = (peak * UNIT).astype(jnp.int32) + 1
    put_peak(units)
    gain = jnp.broadcast_to(
        (REACH * REACH * UNIT) / units.astype(jnp.float32), (8, 8, LANES)
    ).reshape(DIGIT, LANES)
    for pair in range(4):
        low, high = (
            (share * lax.rsqrt(jnp.abs(share) + 1e-30) + 32768.5).astype(jnp.int32)
            for share in (read(pair) * gain, read(pair + 4) * gain)
        )
        put_words(pair, low | jnp.left_shift(high, 16))


def widen(words, peaks, block):
    total = None
    for read_words, peak in zip(words, peaks):
        packed = read_words(block % 4)
        if block < 4:
            numbers = packed & 65535
        else:
            numbers = lax.shift_right_logical(packed, 16)
        root = numbers.astype(jnp.float32) - 32768.0
        term = root * jnp.abs(root) * peak
        total = term if total is None else total + term
    return total


def peak_factor(units):
    factor = units.astype(jnp.float32) * (1.0 / (REACH * REACH * UNIT))
    return jnp.broadcast_to(factor, (8, 8, LANES)).reshape(DIGIT, LANES)


def gather_kernel(part, parts, *refs):
    values, codes = refs[:8], refs[8:16]
    (outs, (low_ref, level_ref, counts_a, counts_b, held, words_ref, scales_ref, sem)) = (
        refs[-12:-8], refs[-8:]
    )
    target = pl.program_id(0)
    slot = lax.rem(target, 2)
    bag = 8
    span = SIDE * bag

    def copies(which, slot):
        rows = SIDE * 256
        return (
            pltpu.make_async_copy(
                words_ref.at[slot], outs[which].at[pl.ds(part * rows, rows), :], sem.at[slot, 0]
            ),
            pltpu.make_async_copy(
                scales_ref.at[slot],
                outs[which].at[pl.ds(parts * rows + part * 8 * SIDE, 8 * SIDE), :],
                sem.at[slot, 1],
            ),
        )

    for k in range(8):
        low, level = decode(codes[k][...].astype(jnp.float32))
        low_ref[k * span:(k + 1) * span, :] = low
        level_ref[k * span:(k + 1) * span, :] = level

    @pl.when(target >= 2)
    def _():
        for copy in copies(0, slot):
            copy.wait()

    def two_tables(couple, carry):
        for t in range(2):
            table = couple * 2 + t
            counts = counts_a if t == 0 else counts_b
            for column in range(8):
                first = column * span + table * bag
                count_rows(low_ref, level_ref, counts, first, column, bag)
            at = pl.ds(pl.multiple_of(table * LANES, LANES), LANES)
            rows = jnp.concatenate([ref[at, :] for ref in values], axis=0)
            held[t] = jnp.dot(counts[...], rows, preferred_element_type=jnp.float32)
        for t in range(2):
            table = couple * 2 + t

            def read(block):
                return held[t, block * DIGIT:(block + 1) * DIGIT, :] * digit_weight(block)

            def put_words(pair, words):
                at = pl.multiple_of(table * 256 + pair * DIGIT, DIGIT)
                words_ref[slot, pl.ds(at, DIGIT), :] = words

            def put_peak(units):
                scales_ref[slot, pl.ds(pl.multiple_of(table * 8, 8), 8), :] = units

            narrow_table(read, put_words, put_peak)
        return carry

    lax.fori_loop(0, 2, two_tables, 0)
    for which in range(SIDE):
        @pl.when(target == which)
        def _():
            for copy in copies(which, slot):
                copy.start()

    @pl.when(target == SIDE - 1)
    def _():
        for copy in copies(0, 1 - slot) + copies(0, slot):
            copy.wait()


def digit_weight(digit):
    return 1.0 if digit == 7 else 1.0 / 16.0**digit


def sum_line(messages, part=0, parts=1, into=()):
    rows, width = messages[0].shape
    samples, bag = LANES, 8
    out = jax.ShapeDtypeStruct((parts * SIDE * 264, width), jnp.int32)
    return pl.pallas_call(
        functools.partial(gather_kernel, part, parts),
        out_shape=(out,) * SIDE,
        grid=(SIDE,),
        in_specs=(
            [pl.BlockSpec((SIDE * samples, width), lambda i: (i, 0))] * 8
            + [pl.BlockSpec((SIDE * bag, width), lambda i: (TILE * samples // (SIDE * bag) + i, 0))] * 8
            + [pl.BlockSpec(memory_space=pl.ANY)] * len(into)
        ),
        out_specs=(pl.BlockSpec(memory_space=pl.ANY),) * SIDE,
        scratch_shapes=[
            pltpu.VMEM((256, LANES), jnp.int32),
            pltpu.VMEM((256, LANES), jnp.int32),
            pltpu.VMEM((512, 1024), jnp.bfloat16),
            pltpu.VMEM((512, 1024), jnp.bfloat16),
            pltpu.VMEM((2, 512, LANES), jnp.float32),
            pltpu.VMEM((2, SIDE * 256, LANES), jnp.int32),
            pltpu.VMEM((2, SIDE * 8, LANES), jnp.int32),
            pltpu.SemaphoreType.DMA((2, 2)),
        ],
        input_output_aliases={16 + n: n for n in range(len(into))},
        compiler_params=pltpu.CompilerParams(dimension_semantics=("arbitrary",)),
        cost_estimate=pl.CostEstimate(
            flops=16 * 2 * 512 * 1024 * 128, bytes_accessed=8 * rows * 256, transcendentals=0
        ),
        name="sum_line",
    )(*messages, *messages, *into)


def merge_kernel(groups, *refs):
    words = refs[:SIDE * groups]
    scales = refs[SIDE * groups:2 * SIDE * groups]
    outs, held, done = refs[-SIDE - 2:-2], refs[-2], refs[-1]
    table = pl.program_id(0)
    for group in range(groups):
        mine = slice(group * SIDE, (group + 1) * SIDE)
        read_words = [
            lambda quarter, ref=ref: ref[quarter * DIGIT:(quarter + 1) * DIGIT, :]
            for ref in words[mine]
        ]
        peaks = [peak_factor(ref[...]) for ref in scales[mine]]
        for block in range(8):
            held[group, block * DIGIT:(block + 1) * DIGIT, :] = widen(read_words, peaks, block)

        def put_words(pair, packed):
            at = group * 264 + pair * DIGIT
            done[at:at + DIGIT, :] = packed

        def put_peak(units):
            done[group * 264 + 256:group * 264 + 264, :] = units

        narrow_table(
            lambda block: held[group, block * DIGIT:(block + 1) * DIGIT, :], put_words, put_peak
        )
    for which in range(SIDE):
        @pl.when(table == which)
        def _():
            outs[which][...] = done[...]


def merge_tables(groups):
    count = len(groups)
    words, scales, arrays = [], [], []
    for line, part, parts in groups:
        arrays += line
        words += [
            pl.BlockSpec((256, LANES), lambda i, p=part: (p * SIDE + i, 0)) for _ in line
        ]
        scales += [
            pl.BlockSpec((8, LANES), lambda i, p=part, n=parts: (n * 128 + p * SIDE + i, 0))
            for _ in line
        ]
    out = jax.ShapeDtypeStruct((count * 264, LANES), jnp.int32)
    return pl.pallas_call(
        functools.partial(merge_kernel, count),
        out_shape=(out,) * SIDE,
        grid=(SIDE,),
        in_specs=words + scales,
        out_specs=(pl.BlockSpec((count * 264, LANES), lambda i: (0, 0)),) * SIDE,
        scratch_shapes=[
            pltpu.VMEM((count, 512, LANES), jnp.float32),
            pltpu.VMEM((count * 264, LANES), jnp.int32),
        ],
        compiler_params=pltpu.CompilerParams(dimension_semantics=("arbitrary",)),
        cost_estimate=pl.CostEstimate(
            flops=count * 20_000_000, bytes_accessed=count * 5 * 532480, transcendentals=0
        ),
        name="merge_tables",
    )(*arrays, *arrays)


def pick_row(rows, index):
    row = lax.broadcasted_iota(jnp.int32, rows.shape, 0)
    return jnp.sum(jnp.where(row == index, rows, 0.0), axis=0, keepdims=True)


def finish_kernel(offsets, quarters, start_ref, *refs):
    count = len(offsets)
    sums, weights = refs[:SIDE * count], refs[SIDE * count:(SIDE + 1) * count]
    accum, out, rows = refs[(SIDE + 1) * count:]
    for n in range(count):
        base = offsets[n] * 264
        mine = sums[n * SIDE:(n + 1) * SIDE]
        read_words = [
            lambda quarter, ref=ref: ref[base + quarter * DIGIT:base + (quarter + 1) * DIGIT, :]
            for ref in mine
        ]
        peaks = [peak_factor(ref[base + 256:base + 264, :]) for ref in mine]
        for block in range(4):
            grad = jnp.concatenate(
                [widen(read_words, peaks, 2 * block), widen(read_words, peaks, 2 * block + 1)],
                axis=0,
            )
            span = slice(block * LANES, (block + 1) * LANES)
            mean = jnp.sum(grad * grad, axis=1, keepdims=True) * (1.0 / LANES)
            new = as_column(pick_row(accum[:, span], start_ref[0] + quarters[n])) + mean
            step_size = LEARN_RATE / (jnp.sqrt(new) + EPSILON)
            old = weights[n][0, span, :].astype(jnp.float32)
            at = n * 528 + block * LANES
            out[at:at + LANES, :] = (old - step_size * grad).astype(out.dtype)
            left = as_row(new)
            for piece in range(3):
                head = left.astype(jnp.bfloat16).astype(jnp.float32)
                rows[piece * 4 + block:piece * 4 + block + 1, :] = head
                left = left - head
        rows[12:16, :] = jnp.zeros((4, LANES), jnp.float32)
        out[n * 528 + 512:n * 528 + 528, :] = rows[...].astype(out.dtype)


def finish(sums, weights, accum, start, quarters):
    count = len(quarters)
    rows = weights.shape[1]
    flat = [piece for line, _ in sums for piece in line]

    def at(q):
        return lambda i, s: (s[0] + q, 0, 0)

    return pl.pallas_call(
        functools.partial(finish_kernel, tuple(offset for _, offset in sums), quarters),
        out_shape=jax.ShapeDtypeStruct((count * 528, LANES), jnp.bfloat16),
        grid_spec=pltpu.PrefetchScalarGridSpec(
            num_scalar_prefetch=1,
            grid=(1,),
            in_specs=(
                [pl.BlockSpec(piece.shape, lambda i, s: (0, 0)) for piece in flat]
                + [pl.BlockSpec((1, rows, LANES), at(q)) for q in quarters]
                + [pl.BlockSpec(accum.shape, lambda i, s: (0, 0))]
            ),
            out_specs=pl.BlockSpec((count * 528, LANES), lambda i, s: (0, 0)),
            scratch_shapes=[pltpu.VMEM((16, LANES), jnp.float32)],
        ),
        compiler_params=pltpu.CompilerParams(dimension_semantics=("arbitrary",)),
        cost_estimate=pl.CostEstimate(
            flops=10_000_000, bytes_accessed=count * 900_000, transcendentals=0
        ),
        name="finish",
    )(start, *flat, *([weights] * count), accum)


def place_kernel(layout, x_ref, *refs):
    ins, (out_w, out_a) = refs[:-2], refs[-2:]
    shape = (out_a.shape[0], LANES)
    row = lax.broadcasted_iota(jnp.int32, shape, 0)
    table = [jnp.zeros(shape, jnp.float32)] * 4
    for group, quarters in enumerate(layout):
        for by in range(SIDE):
            ref = ins[group * SIDE + by]
            base = ((x_ref[0] + SIDE - by) & 3) * SIDE
            for n, q in enumerate(quarters):
                out_w[base + q] = ref[n * 528:n * 528 + 512, :]
                pieces = ref[n * 528 + 512:n * 528 + 528, :].astype(jnp.float32)
                sums = (pieces[0:4, :] + pieces[4:8, :]) + pieces[8:12, :]
                for block in range(4):
                    table[block] = jnp.where(row == base + q, sums[block:block + 1, :], table[block])
    for block in range(4):
        out_a[:, block * LANES:(block + 1) * LANES] = table[block]


def place(messages, layout, x, slots, rows):
    return pl.pallas_call(
        functools.partial(place_kernel, layout),
        out_shape=(
            jax.ShapeDtypeStruct((slots, rows, LANES), jnp.bfloat16),
            jax.ShapeDtypeStruct((slots, rows), jnp.float32),
        ),
        in_specs=[pl.BlockSpec(memory_space=pltpu.SMEM)]
        + [pl.BlockSpec(memory_space=pltpu.VMEM)] * len(messages),
        out_specs=(pl.BlockSpec(memory_space=pltpu.VMEM),) * 2,
        name="place",
    )(x, *messages)


def body(grad_pooled, bag_rows, bag_lengths, table_order, weights, accum):
    x = lax.axis_index("group").astype(jnp.int32)
    shard = lax.axis_index("shard").astype(jnp.int32)
    here = jnp.stack([x, shard // 8, (shard // 2) % 4, shard % 2]).astype(jnp.int32)
    messages = pack_tables(
        grad_pooled, jnp.transpose(bag_rows, (0, 2, 1)), bag_lengths, table_order, here
    )
    arrived = []
    for part, route in enumerate(ROUTES):
        line = []
        for k in range(8):
            sent = messages[part * 8 + k]
            line.append(sent if k == 0 else shift(sent, route[0], k // 2, k % 2))
        arrived.append(line)
    def ring(arrays, axis):
        return [arrays[0]] + [shift(arrays[by], axis, by) for by in range(1, SIDE)]

    lines = [ring(sum_line(arrived[part]), ROUTES[part][1]) for part in range(4)]
    sums_bc = ring(merge_tables([(lines[1], 0, 1), (lines[2], 0, 1)]), "x")
    sums_a = ring(merge_tables([(lines[0], 0, 1)]), "z")
    sums_d = ring(merge_tables([(lines[3], 0, 1)]), "y")
    sums = [(sums_a, 0), (sums_bc, 0), (sums_bc, 1), (sums_d, 0)]
    layout = ((0, 1, 2), (3,))
    start = (x * SIDE).reshape(1)
    final = []
    for quarters in layout:
        mine = finish([sums[q] for q in quarters], weights, accum, start, quarters)
        final += [mine] + [shift(mine, "x", by) for by in range(1, SIDE)]
    new_weights, new_accum = place(
        final, layout, x.reshape(1), weights.shape[0], weights.shape[1]
    )
    return (new_weights, new_accum)


def solution(mesh):
    in_specs = (
        P(("group", "shard"), None, None),
        P(("group", "shard"), None, None),
        P(("group", "shard"), None),
        P(),
        P("shard", None, None),
        P("shard", None),
    )
    out_specs = (P("shard", None, None), P("shard", None))
    return jax.shard_map(body, mesh=mesh, in_specs=in_specs, out_specs=out_specs, check_vma=False)
```

```python
import functools

import jax
import jax.numpy as jnp
from jax import lax
from jax.experimental import pallas as pl
from jax.experimental.pallas import tpu as pltpu
from jax.sharding import PartitionSpec as P

LEARN_RATE = 0.5
EPSILON = 1e-06
LANES = 128
TILE = 16
DIGIT = 64
SIDE = 4
MIB = 1 << 20
AXES = ("group", "shard")
ROUTES = ("xyz", "yzx", "zyx", "xzy")
REACH = 32500.0
UNIT = 1024.0


def device_of(x, z, y, c):
    return x * 32 + (z * SIDE + y) * 2 + c


def shift(value, axis, by, flip=0):
    pairs = []
    for x in range(SIDE):
        for z in range(SIDE):
            for y in range(SIDE):
                for c in range(2):
                    to = {"x": x, "y": y, "z": z}
                    to[axis] = (to[axis] + by) % SIDE
                    pairs.append((device_of(x, z, y, c), device_of(to["x"], to["z"], to["y"], c ^ flip)))
    return lax.ppermute(value, AXES, pairs)


def pack_kernel(order_ref, here_ref, grad_ref, rows_ref, lens_ref, *rest):
    outs, (codes, stage, id_stage, turn_ref, sem) = rest[:32], rest[32:]
    samples, bag, tables = rows_ref.shape
    step = pl.program_id(0)

    @pl.when(step == 0)
    def _():
        shape = (TILE * TILE, TILE * TILE)
        row = lax.broadcasted_iota(jnp.int32, shape, 0)
        source = (row & (TILE - 1)) * TILE + lax.shift_right_logical(row, 4)
        same = source == lax.broadcasted_iota(jnp.int32, shape, 1)
        turn_ref[...] = jnp.where(same, 1.0, 0.0).astype(jnp.bfloat16)

    turn = turn_ref[...]

    def turn_pair(pair, carry):
        at = pl.multiple_of(pair * 2 * TILE, 2 * TILE)
        first = grad_ref[:, pl.ds(at, TILE), :].reshape(TILE * TILE, LANES)
        second = grad_ref[:, pl.ds(at + TILE, TILE), :].reshape(TILE * TILE, LANES)
        both = jnp.concatenate([first, second], axis=1)
        turned = jnp.dot(turn, both, preferred_element_type=jnp.float32).astype(jnp.bfloat16)
        for half in range(2):
            part = turned[:, half * LANES:(half + 1) * LANES].reshape(TILE, TILE, LANES)
            here = pl.ds(pl.multiple_of(step * TILE, TILE), TILE)
            stage[pl.ds(at + half * TILE, TILE), here, :] = part
        return carry

    lax.fori_loop(0, tables // (2 * TILE), turn_pair, 0, unroll=4)

    @pl.when(step == 0)
    def _():
        def encode(block, carry):
            span = pl.ds(pl.multiple_of(block * LANES, LANES), LANES)
            lens = lens_ref[:, span]
            for j in range(bag):
                ids = rows_ref[:, j, span]
                code = jnp.left_shift(DIGIT + (ids & (DIGIT - 1)), ids >> 6)
                code = jnp.where(lens > j, code, 0).astype(jnp.float32)
                codes[pl.ds(block * LANES * bag + j, LANES, stride=bag), :] = code.T
            return carry

        lax.fori_loop(0, tables // LANES, encode, 0)

    def table_at(message, i):
        route = ROUTES[message // 8]
        place = {"x": here_ref[0], "z": here_ref[1], "y": here_ref[2]}
        moves = ((message % 8) // 2, lax.shift_right_logical(i, 2), i & 3)
        for axis, by in zip(route, moves):
            place[axis] = (place[axis] + by) & 3
        core = here_ref[3] ^ (message % 2)
        shard = (place["z"] * SIDE + place["y"]) * 2 + core
        return order_ref[shard * 16 + place["x"] * SIDE + message // 8]

    def table_copy(message, i, table):
        return pltpu.make_async_copy(
            stage.at[table],
            outs[message].at[pl.ds(pl.multiple_of(i * samples, samples), samples), :],
            sem.at[message],
        )

    def id_copy(message):
        return pltpu.make_async_copy(
            id_stage.at[message],
            outs[message].at[pl.ds(TILE * samples, TILE * bag), :],
            sem.at[message],
        )

    @pl.when(step == pl.num_programs(0) - 1)
    def _():
        for message in range(32):
            def send(half, carry):
                pieces = []
                for odd in range(2):
                    i = half * 2 + odd
                    table = table_at(message, i)
                    table_copy(message, i, table).start()
                    pieces.append(codes[pl.ds(pl.multiple_of(table * bag, bag), bag), :])
                both = jnp.concatenate(pieces, axis=0).astype(jnp.bfloat16)
                id_stage[message, pl.ds(pl.multiple_of(half * 2 * bag, 2 * bag), 2 * bag), :] = both
                return carry
            lax.fori_loop(0, TILE // 2, send, 0)
            id_copy(message).start()
        for message in range(32):
            def settle(i, carry):
                table_copy(message, i, 0).wait()
                return carry
            lax.fori_loop(0, TILE, settle, 0)
            id_copy(message).wait()


def pack_tables(grad, rows, lens, order, here):
    samples, tables, width = grad.shape
    bag = rows.shape[1]
    message = jax.ShapeDtypeStruct((TILE * (samples + bag), width), jnp.bfloat16)
    return pl.pallas_call(
        pack_kernel,
        out_shape=(message,) * 32,
        grid_spec=pltpu.PrefetchScalarGridSpec(
            num_scalar_prefetch=2,
            grid=(samples // TILE,),
            in_specs=[
                pl.BlockSpec((TILE, tables, width), lambda i, o, h: (i, 0, 0)),
                pl.BlockSpec((samples, bag, tables), lambda i, o, h: (0, 0, 0)),
                pl.BlockSpec((samples, tables), lambda i, o, h: (0, 0)),
            ],
            out_specs=(pl.BlockSpec(memory_space=pl.ANY),) * 32,
            scratch_shapes=[
                pltpu.VMEM((tables * bag, LANES), jnp.float32),
                pltpu.VMEM((tables, samples, width), jnp.bfloat16),
                pltpu.VMEM((32, TILE * bag, LANES), jnp.bfloat16),
                pltpu.VMEM((TILE * TILE, TILE * TILE), jnp.bfloat16),
                pltpu.SemaphoreType.DMA((32,)),
            ],
        ),
        compiler_params=pltpu.CompilerParams(dimension_semantics=("arbitrary",)),
        name="pack_tables",
    )(order, here, grad, rows, lens)


def decode(code):
    level = jnp.ones(code.shape, jnp.int32)
    big = code >= 1024.0
    code = jnp.where(big, code * 0.0625, code)
    level = jnp.where(big, jnp.left_shift(level, 16), level)
    big = code >= 256.0
    code = jnp.where(big, code * 0.25, code)
    level = jnp.where(big, jnp.left_shift(level, 8), level)
    big = code >= 128.0
    code = jnp.where(big, code * 0.5, code)
    level = jnp.where(big, jnp.left_shift(level, 4), level)
    return code.astype(jnp.int32) - DIGIT, level


def count_rows(low_ref, level_ref, counts, first, column, bag):
    sublane = lax.broadcasted_iota(jnp.int32, (DIGIT, LANES), 0)
    word = jnp.zeros((DIGIT, LANES), jnp.int32)
    for j in range(bag):
        low = low_ref[pl.ds(first + j, DIGIT, stride=0), :]
        level = level_ref[pl.ds(first + j, DIGIT, stride=0), :]
        word = word + jnp.where(low == sublane, level, 0)
    for digit in range(8):
        if digit < 7:
            count = (word & (15 << (4 * digit))).astype(jnp.float32)
        else:
            count = lax.shift_right_logical(word, 28).astype(jnp.float32)
        counts[digit * DIGIT:(digit + 1) * DIGIT, column * LANES:(column + 1) * LANES] = (
            count.astype(jnp.bfloat16)
        )


def diagonal():
    shape = (LANES, LANES)
    return lax.broadcasted_iota(jnp.int32, shape, 0) == lax.broadcasted_iota(jnp.int32, shape, 1)


def as_row(column):
    return jnp.sum(jnp.where(diagonal(), column, 0.0), axis=0, keepdims=True)


def as_column(row):
    return jnp.sum(jnp.where(diagonal(), row, 0.0), axis=1, keepdims=True)


def narrow_table(read, put_words, put_peak):
    peak = None
    for block in range(8):
        values = jnp.abs(read(block)).reshape(8, 8, LANES)
        most = jnp.max(values, axis=0)
        peak = most if peak is None else jnp.maximum(peak, most)
    units = (peak * UNIT).astype(jnp.int32) + 1
    put_peak(units)
    gain = jnp.broadcast_to(
        (REACH * REACH * UNIT) / units.astype(jnp.float32), (8, 8, LANES)
    ).reshape(DIGIT, LANES)
    for pair in range(4):
        low, high = (
            (share * lax.rsqrt(jnp.abs(share) + 1e-30) + 32768.5).astype(jnp.int32)
            for share in (read(pair) * gain, read(pair + 4) * gain)
        )
        put_words(pair, low | jnp.left_shift(high, 16))


def widen(words, peaks, block):
    total = None
    for read_words, peak in zip(words, peaks):
        packed = read_words(block % 4)
        if block < 4:
            numbers = packed & 65535
        else:
            numbers = lax.shift_right_logical(packed, 16)
        root = numbers.astype(jnp.float32) - 32768.0
        term = root * jnp.abs(root) * peak
        total = term if total is None else total + term
    return total


def peak_factor(units):
    factor = units.astype(jnp.float32) * (1.0 / (REACH * REACH * UNIT))
    return jnp.broadcast_to(factor, (8, 8, LANES)).reshape(DIGIT, LANES)


def gather_kernel(part, parts, *refs):
    values, codes = refs[:8], refs[8:16]
    (outs, (low_ref, level_ref, counts_a, counts_b, held, words_ref, scales_ref, sem)) = (
        refs[-12:-8], refs[-8:]
    )
    target = pl.program_id(0)
    slot = lax.rem(target, 2)
    bag = 8
    span = SIDE * bag

    def copies(which, slot):
        rows = SIDE * 256
        return (
            pltpu.make_async_copy(
                words_ref.at[slot], outs[which].at[pl.ds(part * rows, rows), :], sem.at[slot, 0]
            ),
            pltpu.make_async_copy(
                scales_ref.at[slot],
                outs[which].at[pl.ds(parts * rows + part * 8 * SIDE, 8 * SIDE), :],
                sem.at[slot, 1],
            ),
        )

    for k in range(8):
        low, level = decode(codes[k][...].astype(jnp.float32))
        low_ref[k * span:(k + 1) * span, :] = low
        level_ref[k * span:(k + 1) * span, :] = level

    @pl.when(target >= 2)
    def _():
        for copy in copies(0, slot):
            copy.wait()

    def two_tables(couple, carry):
        for t in range(2):
            table = couple * 2 + t
            counts = counts_a if t == 0 else counts_b
            for column in range(8):
                first = column * span + table * bag
                count_rows(low_ref, level_ref, counts, first, column, bag)
            at = pl.ds(pl.multiple_of(table * LANES, LANES), LANES)
            rows = jnp.concatenate([ref[at, :] for ref in values], axis=0)
            held[t] = jnp.dot(counts[...], rows, preferred_element_type=jnp.float32)
        for t in range(2):
            table = couple * 2 + t

            def read(block):
                return held[t, block * DIGIT:(block + 1) * DIGIT, :] * digit_weight(block)

            def put_words(pair, words):
                at = pl.multiple_of(table * 256 + pair * DIGIT, DIGIT)
                words_ref[slot, pl.ds(at, DIGIT), :] = words

            def put_peak(units):
                scales_ref[slot, pl.ds(pl.multiple_of(table * 8, 8), 8), :] = units

            narrow_table(read, put_words, put_peak)
        return carry

    lax.fori_loop(0, 2, two_tables, 0)
    for which in range(SIDE):
        @pl.when(target == which)
        def _():
            for copy in copies(which, slot):
                copy.start()

    @pl.when(target == SIDE - 1)
    def _():
        for copy in copies(0, 1 - slot) + copies(0, slot):
            copy.wait()


def digit_weight(digit):
    return 1.0 if digit == 7 else 1.0 / 16.0**digit


def sum_line(messages, part=0, parts=1, into=()):
    rows, width = messages[0].shape
    samples, bag = LANES, 8
    out = jax.ShapeDtypeStruct((parts * SIDE * 264, width), jnp.int32)
    return pl.pallas_call(
        functools.partial(gather_kernel, part, parts),
        out_shape=(out,) * SIDE,
        grid=(SIDE,),
        in_specs=(
            [pl.BlockSpec((SIDE * samples, width), lambda i: (i, 0))] * 8
            + [pl.BlockSpec((SIDE * bag, width), lambda i: (TILE * samples // (SIDE * bag) + i, 0))] * 8
            + [pl.BlockSpec(memory_space=pl.ANY)] * len(into)
        ),
        out_specs=(pl.BlockSpec(memory_space=pl.ANY),) * SIDE,
        scratch_shapes=[
            pltpu.VMEM((256, LANES), jnp.int32),
            pltpu.VMEM((256, LANES), jnp.int32),
            pltpu.VMEM((512, 1024), jnp.bfloat16),
            pltpu.VMEM((512, 1024), jnp.bfloat16),
            pltpu.VMEM((2, 512, LANES), jnp.float32),
            pltpu.VMEM((2, SIDE * 256, LANES), jnp.int32),
            pltpu.VMEM((2, SIDE * 8, LANES), jnp.int32),
            pltpu.SemaphoreType.DMA((2, 2)),
        ],
        input_output_aliases={16 + n: n for n in range(len(into))},
        compiler_params=pltpu.CompilerParams(dimension_semantics=("arbitrary",), vmem_limit_bytes=12 * MIB),
        cost_estimate=pl.CostEstimate(
            flops=16 * 2 * 512 * 1024 * 128, bytes_accessed=8 * rows * 256, transcendentals=0
        ),
        name="sum_line",
    )(*messages, *messages, *into)


def merge_kernel(groups, *refs):
    words = refs[:SIDE * groups]
    scales = refs[SIDE * groups:2 * SIDE * groups]
    outs, held, done = refs[-SIDE - 2:-2], refs[-2], refs[-1]
    table = pl.program_id(0)
    for group in range(groups):
        mine = slice(group * SIDE, (group + 1) * SIDE)
        read_words = [
            lambda quarter, ref=ref: ref[quarter * DIGIT:(quarter + 1) * DIGIT, :]
            for ref in words[mine]
        ]
        peaks = [peak_factor(ref[...]) for ref in scales[mine]]
        for block in range(8):
            held[group, block * DIGIT:(block + 1) * DIGIT, :] = widen(read_words, peaks, block)

        def put_words(pair, packed):
            at = group * 264 + pair * DIGIT
            done[at:at + DIGIT, :] = packed

        def put_peak(units):
            done[group * 264 + 256:group * 264 + 264, :] = units

        narrow_table(
            lambda block: held[group, block * DIGIT:(block + 1) * DIGIT, :], put_words, put_peak
        )
    for which in range(SIDE):
        @pl.when(table == which)
        def _():
            outs[which][...] = done[...]


def merge_tables(groups):
    count = len(groups)
    words, scales, arrays = [], [], []
    for line, part, parts in groups:
        arrays += line
        words += [
            pl.BlockSpec((256, LANES), lambda i, p=part: (p * SIDE + i, 0)) for _ in line
        ]
        scales += [
            pl.BlockSpec((8, LANES), lambda i, p=part, n=parts: (n * 128 + p * SIDE + i, 0))
            for _ in line
        ]
    out = jax.ShapeDtypeStruct((count * 264, LANES), jnp.int32)
    return pl.pallas_call(
        functools.partial(merge_kernel, count),
        out_shape=(out,) * SIDE,
        grid=(SIDE,),
        in_specs=words + scales,
        out_specs=(pl.BlockSpec((count * 264, LANES), lambda i: (0, 0)),) * SIDE,
        scratch_shapes=[
            pltpu.VMEM((count, 512, LANES), jnp.float32),
            pltpu.VMEM((count * 264, LANES), jnp.int32),
        ],
        compiler_params=pltpu.CompilerParams(dimension_semantics=("arbitrary",), vmem_limit_bytes=8 * MIB),
        cost_estimate=pl.CostEstimate(
            flops=count * 20_000_000, bytes_accessed=count * 5 * 532480, transcendentals=0
        ),
        name="merge_tables",
    )(*arrays, *arrays)


def pick_row(rows, index):
    row = lax.broadcasted_iota(jnp.int32, rows.shape, 0)
    return jnp.sum(jnp.where(row == index, rows, 0.0), axis=0, keepdims=True)


def finish_kernel(offsets, quarters, start_ref, *refs):
    count = len(offsets)
    sums, weights = refs[:SIDE * count], refs[SIDE * count:(SIDE + 1) * count]
    accum, out, rows = refs[(SIDE + 1) * count:]
    for n in range(count):
        base = offsets[n] * 264
        mine = sums[n * SIDE:(n + 1) * SIDE]
        read_words = [
            lambda quarter, ref=ref: ref[base + quarter * DIGIT:base + (quarter + 1) * DIGIT, :]
            for ref in mine
        ]
        peaks = [peak_factor(ref[base + 256:base + 264, :]) for ref in mine]
        for block in range(4):
            grad = jnp.concatenate(
                [widen(read_words, peaks, 2 * block), widen(read_words, peaks, 2 * block + 1)],
                axis=0,
            )
            span = slice(block * LANES, (block + 1) * LANES)
            mean = jnp.sum(grad * grad, axis=1, keepdims=True) * (1.0 / LANES)
            new = as_column(pick_row(accum[:, span], start_ref[0] + quarters[n])) + mean
            step_size = LEARN_RATE / (jnp.sqrt(new) + EPSILON)
            old = weights[n][0, span, :].astype(jnp.float32)
            at = n * 528 + block * LANES
            out[at:at + LANES, :] = (old - step_size * grad).astype(out.dtype)
            left = as_row(new)
            for piece in range(3):
                head = left.astype(jnp.bfloat16).astype(jnp.float32)
                rows[piece * 4 + block:piece * 4 + block + 1, :] = head
                left = left - head
        rows[12:16, :] = jnp.zeros((4, LANES), jnp.float32)
        out[n * 528 + 512:n * 528 + 528, :] = rows[...].astype(out.dtype)


def finish(sums, weights, accum, start, quarters):
    count = len(quarters)
    rows = weights.shape[1]
    flat = [piece for line, _ in sums for piece in line]

    def at(q):
        return lambda i, s: (s[0] + q, 0, 0)

    return pl.pallas_call(
        functools.partial(finish_kernel, tuple(offset for _, offset in sums), quarters),
        out_shape=jax.ShapeDtypeStruct((count * 528, LANES), jnp.bfloat16),
        grid_spec=pltpu.PrefetchScalarGridSpec(
            num_scalar_prefetch=1,
            grid=(1,),
            in_specs=(
                [pl.BlockSpec(piece.shape, lambda i, s: (0, 0)) for piece in flat]
                + [pl.BlockSpec((1, rows, LANES), at(q)) for q in quarters]
                + [pl.BlockSpec(accum.shape, lambda i, s: (0, 0))]
            ),
            out_specs=pl.BlockSpec((count * 528, LANES), lambda i, s: (0, 0)),
            scratch_shapes=[pltpu.VMEM((16, LANES), jnp.float32)],
        ),
        compiler_params=pltpu.CompilerParams(dimension_semantics=("arbitrary",), vmem_limit_bytes=8 * MIB),
        cost_estimate=pl.CostEstimate(
            flops=10_000_000, bytes_accessed=count * 900_000, transcendentals=0
        ),
        name="finish",
    )(start, *flat, *([weights] * count), accum)


def place_kernel(layout, x_ref, *refs):
    ins, (out_w, out_a) = refs[:-2], refs[-2:]
    shape = (out_a.shape[0], LANES)
    row = lax.broadcasted_iota(jnp.int32, shape, 0)
    table = [jnp.zeros(shape, jnp.float32)] * 4
    for group, quarters in enumerate(layout):
        for by in range(SIDE):
            ref = ins[group * SIDE + by]
            base = ((x_ref[0] + SIDE - by) & 3) * SIDE
            for n, q in enumerate(quarters):
                out_w[base + q] = ref[n * 528:n * 528 + 512, :]
                pieces = ref[n * 528 + 512:n * 528 + 528, :].astype(jnp.float32)
                sums = (pieces[0:4, :] + pieces[4:8, :]) + pieces[8:12, :]
                for block in range(4):
                    table[block] = jnp.where(row == base + q, sums[block:block + 1, :], table[block])
    for block in range(4):
        out_a[:, block * LANES:(block + 1) * LANES] = table[block]


def place(messages, layout, x, slots, rows):
    return pl.pallas_call(
        functools.partial(place_kernel, layout),
        out_shape=(
            jax.ShapeDtypeStruct((slots, rows, LANES), jnp.bfloat16),
            jax.ShapeDtypeStruct((slots, rows), jnp.float32),
        ),
        in_specs=[pl.BlockSpec(memory_space=pltpu.SMEM)]
        + [pl.BlockSpec(memory_space=pltpu.VMEM)] * len(messages),
        out_specs=(pl.BlockSpec(memory_space=pltpu.VMEM),) * 2,
        compiler_params=pltpu.CompilerParams(vmem_limit_bytes=8 * MIB),
        name="place",
    )(x, *messages)


def body(grad_pooled, bag_rows, bag_lengths, table_order, weights, accum):
    x = lax.axis_index("group").astype(jnp.int32)
    shard = lax.axis_index("shard").astype(jnp.int32)
    here = jnp.stack([x, shard // 8, (shard // 2) % 4, shard % 2]).astype(jnp.int32)
    messages = pack_tables(
        grad_pooled, jnp.transpose(bag_rows, (0, 2, 1)), bag_lengths, table_order, here
    )
    arrived = []
    for part, route in enumerate(ROUTES):
        line = []
        for k in range(8):
            sent = messages[part * 8 + k]
            line.append(sent if k == 0 else shift(sent, route[0], k // 2, k % 2))
        arrived.append(line)
    def ring(arrays, axis):
        return [arrays[0]] + [shift(arrays[by], axis, by) for by in range(1, SIDE)]

    lines = [ring(sum_line(arrived[part]), ROUTES[part][1]) for part in range(4)]
    sums_bc = ring(merge_tables([(lines[1], 0, 1), (lines[2], 0, 1)]), "x")
    sums_a = ring(merge_tables([(lines[0], 0, 1)]), "z")
    sums_d = ring(merge_tables([(lines[3], 0, 1)]), "y")
    sums = [(sums_a, 0), (sums_bc, 0), (sums_bc, 1), (sums_d, 0)]
    layout = ((0, 1, 2), (3,))
    start = (x * SIDE).reshape(1)
    final = []
    for quarters in layout:
        mine = finish([sums[q] for q in quarters], weights, accum, start, quarters)
        final += [mine] + [shift(mine, "x", by) for by in range(1, SIDE)]
    new_weights, new_accum = place(
        final, layout, x.reshape(1), weights.shape[0], weights.shape[1]
    )
    return (new_weights, new_accum)


def solution(mesh):
    in_specs = (
        P(("group", "shard"), None, None),
        P(("group", "shard"), None, None),
        P(("group", "shard"), None),
        P(),
        P("shard", None, None),
        P("shard", None),
    )
    out_specs = (P("shard", None, None), P("shard", None))
    return jax.shard_map(body, mesh=mesh, in_specs=in_specs, out_specs=out_specs, check_vma=False)
```

```python
import functools

import jax
import jax.numpy as jnp
from jax import lax
from jax.experimental import pallas as pl
from jax.experimental.pallas import tpu as pltpu
from jax.sharding import PartitionSpec as P

LEARN_RATE = 0.5
EPSILON = 1e-06
LANES = 128
TILE = 16
DIGIT = 64
SIDE = 4
MIB = 1 << 20
AXES = ("group", "shard")
ROUTES = ("xyz", "yzx", "zyx", "xyz")
REACH = 32500.0
UNIT = 1024.0


def device_of(x, z, y, c):
    return x * 32 + (z * SIDE + y) * 2 + c


def shift(value, axis, by, flip=0):
    pairs = []
    for x in range(SIDE):
        for z in range(SIDE):
            for y in range(SIDE):
                for c in range(2):
                    to = {"x": x, "y": y, "z": z}
                    to[axis] = (to[axis] + by) % SIDE
                    pairs.append((device_of(x, z, y, c), device_of(to["x"], to["z"], to["y"], c ^ flip)))
    return lax.ppermute(value, AXES, pairs)


def pack_kernel(order_ref, here_ref, grad_ref, rows_ref, lens_ref, *rest):
    outs, (codes, stage, id_stage, turn_ref, sem) = rest[:32], rest[32:]
    samples, bag, tables = rows_ref.shape
    step = pl.program_id(0)

    @pl.when(step == 0)
    def _():
        shape = (TILE * TILE, TILE * TILE)
        row = lax.broadcasted_iota(jnp.int32, shape, 0)
        source = (row & (TILE - 1)) * TILE + lax.shift_right_logical(row, 4)
        same = source == lax.broadcasted_iota(jnp.int32, shape, 1)
        turn_ref[...] = jnp.where(same, 1.0, 0.0).astype(jnp.bfloat16)

    turn = turn_ref[...]

    def turn_pair(pair, carry):
        at = pl.multiple_of(pair * 2 * TILE, 2 * TILE)
        first = grad_ref[:, pl.ds(at, TILE), :].reshape(TILE * TILE, LANES)
        second = grad_ref[:, pl.ds(at + TILE, TILE), :].reshape(TILE * TILE, LANES)
        both = jnp.concatenate([first, second], axis=1)
        turned = jnp.dot(turn, both, preferred_element_type=jnp.float32).astype(jnp.bfloat16)
        for half in range(2):
            part = turned[:, half * LANES:(half + 1) * LANES].reshape(TILE, TILE, LANES)
            here = pl.ds(pl.multiple_of(step * TILE, TILE), TILE)
            stage[pl.ds(at + half * TILE, TILE), here, :] = part
        return carry

    lax.fori_loop(0, tables // (2 * TILE), turn_pair, 0, unroll=4)

    @pl.when(step == 0)
    def _():
        def encode(block, carry):
            span = pl.ds(pl.multiple_of(block * LANES, LANES), LANES)
            lens = lens_ref[:, span]
            for j in range(bag):
                ids = rows_ref[:, j, span]
                code = jnp.left_shift(DIGIT + (ids & (DIGIT - 1)), ids >> 6)
                code = jnp.where(lens > j, code, 0).astype(jnp.float32)
                codes[pl.ds(block * LANES * bag + j, LANES, stride=bag), :] = code.T
            return carry

        lax.fori_loop(0, tables // LANES, encode, 0)

    def table_at(message, i):
        route = ROUTES[message // 8]
        place = {"x": here_ref[0], "z": here_ref[1], "y": here_ref[2]}
        moves = ((message % 8) // 2, lax.shift_right_logical(i, 2), i & 3)
        for axis, by in zip(route, moves):
            place[axis] = (place[axis] + by) & 3
        core = here_ref[3] ^ (message % 2)
        shard = (place["z"] * SIDE + place["y"]) * 2 + core
        return order_ref[shard * 16 + place["x"] * SIDE + message // 8]

    def table_copy(message, i, table):
        return pltpu.make_async_copy(
            stage.at[table],
            outs[message].at[pl.ds(pl.multiple_of(i * samples, samples), samples), :],
            sem.at[message],
        )

    def id_copy(message):
        return pltpu.make_async_copy(
            id_stage.at[message],
            outs[message].at[pl.ds(TILE * samples, TILE * bag), :],
            sem.at[message],
        )

    @pl.when(step == pl.num_programs(0) - 1)
    def _():
        for message in range(32):
            def send(half, carry):
                pieces = []
                for odd in range(2):
                    i = half * 2 + odd
                    table = table_at(message, i)
                    table_copy(message, i, table).start()
                    pieces.append(codes[pl.ds(pl.multiple_of(table * bag, bag), bag), :])
                both = jnp.concatenate(pieces, axis=0).astype(jnp.bfloat16)
                id_stage[message, pl.ds(pl.multiple_of(half * 2 * bag, 2 * bag), 2 * bag), :] = both
                return carry
            lax.fori_loop(0, TILE // 2, send, 0)
            id_copy(message).start()
        for message in range(32):
            def settle(i, carry):
                table_copy(message, i, 0).wait()
                return carry
            lax.fori_loop(0, TILE, settle, 0)
            id_copy(message).wait()


def pack_tables(grad, rows, lens, order, here):
    samples, tables, width = grad.shape
    bag = rows.shape[1]
    message = jax.ShapeDtypeStruct((TILE * (samples + bag), width), jnp.bfloat16)
    return pl.pallas_call(
        pack_kernel,
        out_shape=(message,) * 32,
        grid_spec=pltpu.PrefetchScalarGridSpec(
            num_scalar_prefetch=2,
            grid=(samples // TILE,),
            in_specs=[
                pl.BlockSpec((TILE, tables, width), lambda i, o, h: (i, 0, 0)),
                pl.BlockSpec((samples, bag, tables), lambda i, o, h: (0, 0, 0)),
                pl.BlockSpec((samples, tables), lambda i, o, h: (0, 0)),
            ],
            out_specs=(pl.BlockSpec(memory_space=pl.ANY),) * 32,
            scratch_shapes=[
                pltpu.VMEM((tables * bag, LANES), jnp.float32),
                pltpu.VMEM((tables, samples, width), jnp.bfloat16),
                pltpu.VMEM((32, TILE * bag, LANES), jnp.bfloat16),
                pltpu.VMEM((TILE * TILE, TILE * TILE), jnp.bfloat16),
                pltpu.SemaphoreType.DMA((32,)),
            ],
        ),
        compiler_params=pltpu.CompilerParams(dimension_semantics=("arbitrary",)),
        name="pack_tables",
    )(order, here, grad, rows, lens)


def decode(code):
    level = jnp.ones(code.shape, jnp.int32)
    big = code >= 1024.0
    code = jnp.where(big, code * 0.0625, code)
    level = jnp.where(big, jnp.left_shift(level, 16), level)
    big = code >= 256.0
    code = jnp.where(big, code * 0.25, code)
    level = jnp.where(big, jnp.left_shift(level, 8), level)
    big = code >= 128.0
    code = jnp.where(big, code * 0.5, code)
    level = jnp.where(big, jnp.left_shift(level, 4), level)
    return code.astype(jnp.int32) - DIGIT, level


def count_rows(low_ref, level_ref, counts, first, column, bag):
    sublane = lax.broadcasted_iota(jnp.int32, (DIGIT, LANES), 0)
    word = jnp.zeros((DIGIT, LANES), jnp.int32)
    for j in range(bag):
        low = low_ref[pl.ds(first + j, DIGIT, stride=0), :]
        level = level_ref[pl.ds(first + j, DIGIT, stride=0), :]
        word = word + jnp.where(low == sublane, level, 0)
    for digit in range(8):
        if digit < 7:
            count = (word & (15 << (4 * digit))).astype(jnp.float32)
        else:
            count = lax.shift_right_logical(word, 28).astype(jnp.float32)
        counts[digit * DIGIT:(digit + 1) * DIGIT, column * LANES:(column + 1) * LANES] = (
            count.astype(jnp.bfloat16)
        )


def diagonal():
    shape = (LANES, LANES)
    return lax.broadcasted_iota(jnp.int32, shape, 0) == lax.broadcasted_iota(jnp.int32, shape, 1)


def as_row(column):
    return jnp.sum(jnp.where(diagonal(), column, 0.0), axis=0, keepdims=True)


def as_column(row):
    return jnp.sum(jnp.where(diagonal(), row, 0.0), axis=1, keepdims=True)


def narrow_table(read, put_words, put_peak):
    peak = None
    for block in range(8):
        values = jnp.abs(read(block)).reshape(8, 8, LANES)
        most = jnp.max(values, axis=0)
        peak = most if peak is None else jnp.maximum(peak, most)
    units = (peak * UNIT).astype(jnp.int32) + 1
    put_peak(units)
    gain = jnp.broadcast_to(
        (REACH * REACH * UNIT) / units.astype(jnp.float32), (8, 8, LANES)
    ).reshape(DIGIT, LANES)
    for pair in range(4):
        low, high = (
            (share * lax.rsqrt(jnp.abs(share) + 1e-30) + 32768.5).astype(jnp.int32)
            for share in (read(pair) * gain, read(pair + 4) * gain)
        )
        put_words(pair, low | jnp.left_shift(high, 16))


def widen(words, peaks, block):
    total = None
    for read_words, peak in zip(words, peaks):
        packed = read_words(block % 4)
        if block < 4:
            numbers = packed & 65535
        else:
            numbers = lax.shift_right_logical(packed, 16)
        root = numbers.astype(jnp.float32) - 32768.0
        term = root * jnp.abs(root) * peak
        total = term if total is None else total + term
    return total


def peak_factor(units):
    factor = units.astype(jnp.float32) * (1.0 / (REACH * REACH * UNIT))
    return jnp.broadcast_to(factor, (8, 8, LANES)).reshape(DIGIT, LANES)


def gather_kernel(part, parts, *refs):
    values, codes = refs[:8], refs[8:16]
    (outs, (low_ref, level_ref, counts_a, counts_b, held, words_ref, scales_ref, sem)) = (
        refs[-12:-8], refs[-8:]
    )
    target = pl.program_id(0)
    slot = lax.rem(target, 2)
    bag = 8
    span = SIDE * bag

    def copies(which, slot):
        rows = SIDE * 256
        return (
            pltpu.make_async_copy(
                words_ref.at[slot], outs[which].at[pl.ds(part * rows, rows), :], sem.at[slot, 0]
            ),
            pltpu.make_async_copy(
                scales_ref.at[slot],
                outs[which].at[pl.ds(parts * rows + part * 8 * SIDE, 8 * SIDE), :],
                sem.at[slot, 1],
            ),
        )

    for k in range(8):
        low, level = decode(codes[k][...].astype(jnp.float32))
        low_ref[k * span:(k + 1) * span, :] = low
        level_ref[k * span:(k + 1) * span, :] = level

    @pl.when(target >= 2)
    def _():
        for copy in copies(0, slot):
            copy.wait()

    def two_tables(couple, carry):
        for t in range(2):
            table = couple * 2 + t
            counts = counts_a if t == 0 else counts_b
            for column in range(8):
                first = column * span + table * bag
                count_rows(low_ref, level_ref, counts, first, column, bag)
            at = pl.ds(pl.multiple_of(table * LANES, LANES), LANES)
            rows = jnp.concatenate([ref[at, :] for ref in values], axis=0)
            held[t] = jnp.dot(counts[...], rows, preferred_element_type=jnp.float32)
        for t in range(2):
            table = couple * 2 + t

            def read(block):
                return held[t, block * DIGIT:(block + 1) * DIGIT, :] * digit_weight(block)

            def put_words(pair, words):
                at = pl.multiple_of(table * 256 + pair * DIGIT, DIGIT)
                words_ref[slot, pl.ds(at, DIGIT), :] = words

            def put_peak(units):
                scales_ref[slot, pl.ds(pl.multiple_of(table * 8, 8), 8), :] = units

            narrow_table(read, put_words, put_peak)
        return carry

    lax.fori_loop(0, 2, two_tables, 0)
    for which in range(SIDE):
        @pl.when(target == which)
        def _():
            for copy in copies(which, slot):
                copy.start()

    @pl.when(target == SIDE - 1)
    def _():
        for copy in copies(0, 1 - slot) + copies(0, slot):
            copy.wait()


def digit_weight(digit):
    return 1.0 if digit == 7 else 1.0 / 16.0**digit


def sum_line(messages, part=0, parts=1, into=(), after=()):
    rows, width = messages[0].shape
    samples, bag = LANES, 8
    out = jax.ShapeDtypeStruct((parts * SIDE * 264, width), jnp.int32)
    return pl.pallas_call(
        functools.partial(gather_kernel, part, parts),
        out_shape=(out,) * SIDE,
        grid=(SIDE,),
        in_specs=(
            [pl.BlockSpec((SIDE * samples, width), lambda i: (i, 0))] * 8
            + [pl.BlockSpec((SIDE * bag, width), lambda i: (TILE * samples // (SIDE * bag) + i, 0))] * 8
            + [pl.BlockSpec(memory_space=pl.ANY)] * (len(into) + len(after))
        ),
        out_specs=(pl.BlockSpec(memory_space=pl.ANY),) * SIDE,
        scratch_shapes=[
            pltpu.VMEM((256, LANES), jnp.int32),
            pltpu.VMEM((256, LANES), jnp.int32),
            pltpu.VMEM((512, 1024), jnp.bfloat16),
            pltpu.VMEM((512, 1024), jnp.bfloat16),
            pltpu.VMEM((2, 512, LANES), jnp.float32),
            pltpu.VMEM((2, SIDE * 256, LANES), jnp.int32),
            pltpu.VMEM((2, SIDE * 8, LANES), jnp.int32),
            pltpu.SemaphoreType.DMA((2, 2)),
        ],
        input_output_aliases={16 + n: n for n in range(len(into))},
        compiler_params=pltpu.CompilerParams(dimension_semantics=("arbitrary",), vmem_limit_bytes=12 * MIB),
        cost_estimate=pl.CostEstimate(
            flops=16 * 2 * 512 * 1024 * 128, bytes_accessed=8 * rows * 256, transcendentals=0
        ),
        name="sum_line",
    )(*messages, *messages, *into, *after)


def merge_kernel(groups, *refs):
    words = refs[:SIDE * groups]
    scales = refs[SIDE * groups:2 * SIDE * groups]
    outs, held, done = refs[-SIDE - 2:-2], refs[-2], refs[-1]
    table = pl.program_id(0)
    for group in range(groups):
        mine = slice(group * SIDE, (group + 1) * SIDE)
        read_words = [
            lambda quarter, ref=ref: ref[quarter * DIGIT:(quarter + 1) * DIGIT, :]
            for ref in words[mine]
        ]
        peaks = [peak_factor(ref[...]) for ref in scales[mine]]
        for block in range(8):
            held[group, block * DIGIT:(block + 1) * DIGIT, :] = widen(read_words, peaks, block)

        def put_words(pair, packed):
            at = group * 264 + pair * DIGIT
            done[at:at + DIGIT, :] = packed

        def put_peak(units):
            done[group * 264 + 256:group * 264 + 264, :] = units

        narrow_table(
            lambda block: held[group, block * DIGIT:(block + 1) * DIGIT, :], put_words, put_peak
        )
    for which in range(SIDE):
        @pl.when(table == which)
        def _():
            outs[which][...] = done[...]


def merge_tables(groups):
    count = len(groups)
    words, scales, arrays = [], [], []
    for line, part, parts in groups:
        arrays += line
        words += [
            pl.BlockSpec((256, LANES), lambda i, p=part: (p * SIDE + i, 0)) for _ in line
        ]
        scales += [
            pl.BlockSpec((8, LANES), lambda i, p=part, n=parts: (n * 128 + p * SIDE + i, 0))
            for _ in line
        ]
    out = jax.ShapeDtypeStruct((count * 264, LANES), jnp.int32)
    return pl.pallas_call(
        functools.partial(merge_kernel, count),
        out_shape=(out,) * SIDE,
        grid=(SIDE,),
        in_specs=words + scales,
        out_specs=(pl.BlockSpec((count * 264, LANES), lambda i: (0, 0)),) * SIDE,
        scratch_shapes=[
            pltpu.VMEM((count, 512, LANES), jnp.float32),
            pltpu.VMEM((count * 264, LANES), jnp.int32),
        ],
        compiler_params=pltpu.CompilerParams(dimension_semantics=("arbitrary",), vmem_limit_bytes=8 * MIB),
        cost_estimate=pl.CostEstimate(
            flops=count * 20_000_000, bytes_accessed=count * 5 * 532480, transcendentals=0
        ),
        name="merge_tables",
    )(*arrays, *arrays)


def pick_row(rows, index):
    row = lax.broadcasted_iota(jnp.int32, rows.shape, 0)
    return jnp.sum(jnp.where(row == index, rows, 0.0), axis=0, keepdims=True)


def finish_kernel(offsets, quarters, start_ref, *refs):
    count = len(offsets)
    sums, weights = refs[:SIDE * count], refs[SIDE * count:(SIDE + 1) * count]
    accum, out, rows = refs[(SIDE + 1) * count:]
    for n in range(count):
        base = offsets[n] * 264
        mine = sums[n * SIDE:(n + 1) * SIDE]
        read_words = [
            lambda quarter, ref=ref: ref[base + quarter * DIGIT:base + (quarter + 1) * DIGIT, :]
            for ref in mine
        ]
        peaks = [peak_factor(ref[base + 256:base + 264, :]) for ref in mine]
        for block in range(4):
            grad = jnp.concatenate(
                [widen(read_words, peaks, 2 * block), widen(read_words, peaks, 2 * block + 1)],
                axis=0,
            )
            span = slice(block * LANES, (block + 1) * LANES)
            mean = jnp.sum(grad * grad, axis=1, keepdims=True) * (1.0 / LANES)
            new = as_column(pick_row(accum[:, span], start_ref[0] + quarters[n])) + mean
            step_size = LEARN_RATE / (jnp.sqrt(new) + EPSILON)
            old = weights[n][0, span, :].astype(jnp.float32)
            at = n * 528 + block * LANES
            out[at:at + LANES, :] = (old - step_size * grad).astype(out.dtype)
            left = as_row(new)
            for piece in range(3):
                head = left.astype(jnp.bfloat16).astype(jnp.float32)
                rows[piece * 4 + block:piece * 4 + block + 1, :] = head
                left = left - head
        rows[12:16, :] = jnp.zeros((4, LANES), jnp.float32)
        out[n * 528 + 512:n * 528 + 528, :] = rows[...].astype(out.dtype)


def finish(sums, weights, accum, start, quarters):
    count = len(quarters)
    rows = weights.shape[1]
    flat = [piece for line, _ in sums for piece in line]

    def at(q):
        return lambda i, s: (s[0] + q, 0, 0)

    return pl.pallas_call(
        functools.partial(finish_kernel, tuple(offset for _, offset in sums), quarters),
        out_shape=jax.ShapeDtypeStruct((count * 528, LANES), jnp.bfloat16),
        grid_spec=pltpu.PrefetchScalarGridSpec(
            num_scalar_prefetch=1,
            grid=(1,),
            in_specs=(
                [pl.BlockSpec(piece.shape, lambda i, s: (0, 0)) for piece in flat]
                + [pl.BlockSpec((1, rows, LANES), at(q)) for q in quarters]
                + [pl.BlockSpec(accum.shape, lambda i, s: (0, 0))]
            ),
            out_specs=pl.BlockSpec((count * 528, LANES), lambda i, s: (0, 0)),
            scratch_shapes=[pltpu.VMEM((16, LANES), jnp.float32)],
        ),
        compiler_params=pltpu.CompilerParams(dimension_semantics=("arbitrary",), vmem_limit_bytes=8 * MIB),
        cost_estimate=pl.CostEstimate(
            flops=10_000_000, bytes_accessed=count * 900_000, transcendentals=0
        ),
        name="finish",
    )(start, *flat, *([weights] * count), accum)


def place_kernel(layout, x_ref, *refs):
    ins, (out_w, out_a) = refs[:-2], refs[-2:]
    shape = (out_a.shape[0], LANES)
    row = lax.broadcasted_iota(jnp.int32, shape, 0)
    table = [jnp.zeros(shape, jnp.float32)] * 4
    for group, quarters in enumerate(layout):
        for by in range(SIDE):
            ref = ins[group * SIDE + by]
            base = ((x_ref[0] + SIDE - by) & 3) * SIDE
            for n, q in enumerate(quarters):
                out_w[base + q] = ref[n * 528:n * 528 + 512, :]
                pieces = ref[n * 528 + 512:n * 528 + 528, :].astype(jnp.float32)
                sums = (pieces[0:4, :] + pieces[4:8, :]) + pieces[8:12, :]
                for block in range(4):
                    table[block] = jnp.where(row == base + q, sums[block:block + 1, :], table[block])
    for block in range(4):
        out_a[:, block * LANES:(block + 1) * LANES] = table[block]


def place(messages, layout, x, slots, rows):
    return pl.pallas_call(
        functools.partial(place_kernel, layout),
        out_shape=(
            jax.ShapeDtypeStruct((slots, rows, LANES), jnp.bfloat16),
            jax.ShapeDtypeStruct((slots, rows), jnp.float32),
        ),
        in_specs=[pl.BlockSpec(memory_space=pltpu.SMEM)]
        + [pl.BlockSpec(memory_space=pltpu.VMEM)] * len(messages),
        out_specs=(pl.BlockSpec(memory_space=pltpu.VMEM),) * 2,
        compiler_params=pltpu.CompilerParams(vmem_limit_bytes=8 * MIB),
        name="place",
    )(x, *messages)


def body(grad_pooled, bag_rows, bag_lengths, table_order, weights, accum):
    x = lax.axis_index("group").astype(jnp.int32)
    shard = lax.axis_index("shard").astype(jnp.int32)
    here = jnp.stack([x, shard // 8, (shard // 2) % 4, shard % 2]).astype(jnp.int32)
    messages = pack_tables(
        grad_pooled, jnp.transpose(bag_rows, (0, 2, 1)), bag_lengths, table_order, here
    )
    arrived = []
    for part, route in enumerate(ROUTES):
        line = []
        for k in range(8):
            sent = messages[part * 8 + k]
            line.append(sent if k == 0 else shift(sent, route[0], k // 2, k % 2))
        arrived.append(line)
    def ring(arrays, axis):
        return [arrays[0]] + [shift(arrays[by], axis, by) for by in range(1, SIDE)]

    lines = [ring(sum_line(arrived[part]), ROUTES[part][1]) for part in range(3)]
    merged_bc = merge_tables([(lines[1], 0, 1), (lines[2], 0, 1)])
    lines.append(ring(sum_line(arrived[3], after=(merged_bc[0],)), ROUTES[3][1]))
    sums_bc = ring(merged_bc, "x")
    sums_a = ring(merge_tables([(lines[0], 0, 1)]), ROUTES[0][2])
    sums_d = ring(merge_tables([(lines[3], 0, 1)]), ROUTES[3][2])
    sums = [(sums_a, 0), (sums_bc, 0), (sums_bc, 1), (sums_d, 0)]
    layout = ((0, 1, 2), (3,))
    start = (x * SIDE).reshape(1)
    final = []
    for quarters in layout:
        mine = finish([sums[q] for q in quarters], weights, accum, start, quarters)
        final += [mine] + [shift(mine, "x", by) for by in range(1, SIDE)]
    new_weights, new_accum = place(
        final, layout, x.reshape(1), weights.shape[0], weights.shape[1]
    )
    return (new_weights, new_accum)


def solution(mesh):
    in_specs = (
        P(("group", "shard"), None, None),
        P(("group", "shard"), None, None),
        P(("group", "shard"), None),
        P(),
        P("shard", None, None),
        P("shard", None),
    )
    out_specs = (P("shard", None, None), P("shard", None))
    return jax.shard_map(body, mesh=mesh, in_specs=in_specs, out_specs=out_specs, check_vma=False)
```
